32 devices in a mesh: kv: 2 (over x), dup: 16 (over z, y, core).
Axes of the slice: x: 2, y: 2, z: 4, core: 2. Of those that a mesh axis runs over, the one named last changes fastest.
Arguments:
- queries: bfloat16 [512, 48, 128], P('kv', 'dup'), parts along dimension 0
- key_cache: bfloat16 [512, 4096, 128], P('kv', 'dup'), parts along dimension 0
- value_cache: bfloat16 [512, 4096, 128], P('kv', 'dup'), parts along dimension 0
- lengths: int32 [512], P('kv'), parts along dimension 0
Outputs:
- output: bfloat16 [512, 48, 128], P('kv', 'dup'), parts along dimension 0
There are 2 independent parts. The reference program is written for one: setup_inputs(seed, part) draws one part's arguments, and reference() takes and returns one part's arrays. A program takes and returns all parts, laid end to end along the dimension named above; each array names one.
All inputs are finite; a program needn't handle non-finite values.
Results may differ from the reference program's by a relative error of at most 0.00813525.
Values are sent between devices in bfloat16 or wider.
A program may use at most 1 GiB of HBM per device.

```python
import math
import jax
import jax.numpy as jnp
from jax import lax

BATCH = 256
SEQ = 4096
HEADS = 96
KV_HEADS = 8
HEAD_DIM = 128
DRAFT = 4

GROUP_HEADS = HEADS // KV_HEADS
QUERY_ROWS = GROUP_HEADS * DRAFT


def wave_field(k_freq, k_phase, k_dir, strength):
    spot_frac = jnp.arange(SEQ, dtype=jnp.float32) / SEQ
    freq_row = jax.random.randint(k_freq, (BATCH, 3), 1, 17, jnp.int32).astype(jnp.float32)
    phases = jax.random.uniform(k_phase, (BATCH, 3), jnp.float32) * (2.0 * math.pi)
    directions = jax.random.normal(k_dir, (BATCH, 3, HEAD_DIM), jnp.float32)
    wave_vals = jnp.cos(2.0 * math.pi * freq_row[:, None, :] * spot_frac[None, :, None] + phases[:, None, :])
    return strength * jnp.einsum("bsk,bkd->bsd", wave_vals, directions)


def setup_inputs(seed: int = 0, part: int = 0) -> dict:
    part_key = jax.random.fold_in(jax.random.key(seed), part)
    key_list = jax.random.split(part_key, 11)
    queries = jax.random.normal(key_list[0], (BATCH, QUERY_ROWS, HEAD_DIM), jnp.float32)
    k_noise = jax.random.normal(key_list[1], (BATCH, SEQ, HEAD_DIM), jnp.float32)
    key_cache = k_noise + wave_field(key_list[2], key_list[3], key_list[4], 1.5)
    v_noise = jax.random.normal(key_list[5], (BATCH, SEQ, HEAD_DIM), jnp.float32)
    value_cache = v_noise + wave_field(key_list[6], key_list[7], key_list[8], 1.0)
    low_len = max(DRAFT, SEQ // 8)
    lengths = jax.random.randint(key_list[9], (BATCH,), low_len, SEQ + 1, jnp.int32)
    full_row = jax.random.randint(key_list[10], (), 0, BATCH, jnp.int32)
    lengths = jnp.where(jnp.arange(BATCH) == full_row, SEQ, lengths).astype(jnp.int32)
    return {"queries": queries.astype(jnp.bfloat16), "key_cache": key_cache.astype(jnp.bfloat16), "value_cache": value_cache.astype(jnp.bfloat16), "lengths": lengths}


def reference(queries, key_cache, value_cache, lengths):
    score_scale = 1.0 / math.sqrt(HEAD_DIM)
    draft_pos = jnp.arange(QUERY_ROWS) % DRAFT
    seq_pos = jnp.arange(SEQ)

    def one_sequence(operands):
        q_rows, k_rows, v_rows, length = operands
        scores = jnp.dot(q_rows, k_rows.T, preferred_element_type=jnp.float32) * score_scale
        last_pos = length - DRAFT + draft_pos
        allowed = seq_pos[None, :] <= last_pos[:, None]
        scores = jnp.where(allowed, scores, -jnp.inf)
        row_peak = jnp.max(scores, axis=1, keepdims=True)
        prob_vals = jnp.exp(scores - row_peak)
        row_mass = jnp.sum(prob_vals, axis=1, keepdims=True)
        weighted = jnp.dot(prob_vals.astype(jnp.bfloat16), v_rows, preferred_element_type=jnp.float32)
        return (weighted / row_mass).astype(jnp.bfloat16)

    return lax.map(one_sequence, (queries, key_cache, value_cache, lengths))
```

```python
import functools
import math

import jax
import jax.numpy as jnp
from jax import lax
from jax.experimental import pallas as pl
from jax.experimental.pallas import tpu as pltpu
from jax.sharding import PartitionSpec as P

DRAFT = 4
CHUNKS = 8
UNROLL = 4
NEG = -3.4e38
FLOOR = -3.0e38
MESH = pl.DeviceIdType.MESH
F32 = jnp.float32
BF16 = jnp.bfloat16


def fused(nb, own, span, dim, len_ref, q_ref, k_ref, v_ref, out_ref,
          kbuf, vbuf, qbuf, qf, of, posm, macc, laccs,
          p1s, p1r, e1s, e1k, e1r, p2s, p2k, p2r, e2s, e2k, e2r, p3s, p3k, p3r, e3s, e3k, e3r,
          wtmp, kvsem, qsem, gs, gr, rs, rr):
    nc = CHUNKS
    bc = nb // nc
    pitch = bc + 8
    rows = 16 * own
    half, quar = rows // 2, rows // 4
    scale = dim ** -0.5
    me = lax.axis_index("dup")
    core, yy, zz = me % 2, (me // 2) % 2, me // 4
    partner = me + 1 - 2 * core
    ypeer = me + 2 - 4 * yy
    zpeer = [None,
             me + 4 * (1 - 2 * (zz % 2)),
             me + 4 * (2 - 4 * (zz // 2)),
             me + 4 * (3 - 2 * zz)]

    def kv_copies(c):
        sl = pl.ds(c * bc, bc)
        return (pltpu.make_async_copy(k_ref.at[sl], kbuf.at[sl], kvsem.at[0, c]),
                pltpu.make_async_copy(v_ref.at[sl], vbuf.at[sl], kvsem.at[1, c]))

    def own_q(c):
        return pltpu.make_async_copy(q_ref.at[:, pl.ds(c * bc, bc)], qbuf.at[c, 0], qsem.at[c])

    def remote(src, dst, ssem, rsem, dev):
        return pltpu.make_async_remote_copy(src_ref=src, dst_ref=dst, send_sem=ssem, recv_sem=rsem,
                                            device_id={"dup": dev}, device_id_type=MESH)

    def send_own(c, slot, dev, idx):
        return remote(q_ref.at[:, pl.ds(c * bc, bc)], qbuf.at[c, slot], gs.at[idx, c], gr.at[slot, c], dev)

    def forward(c, slot_from, slot_to, dev, idx):
        return remote(qbuf.at[c, slot_from], qbuf.at[c, slot_to], gs.at[idx, c], gr.at[slot_to, c], dev)

    def own_sends(c):
        return ([send_own(c, k, zpeer[k], k) for k in (1, 2, 3)]
                + [send_own(c, 4, ypeer, 4), send_own(c, 8, partner, 8)])

    def z_forwards(c, k):
        return [forward(c, k, 4 + k, ypeer, 4 + k), forward(c, k, 8 + k, partner, 8 + k)]

    def y_forwards(c, k):
        return [forward(c, 4 + k, 12 + k, partner, 12 + k)]

    def wait_slot(c, slot):
        forward(c, slot, slot, partner, 0).wait_recv()

    def r1_copies(c):
        return [remote(p1s.at[c], p1r.at[c], rs.at[0, c], rr.at[0, c], partner),
                remote(e1s.at[c], e1r.at[c], rs.at[1, c], rr.at[1, c], partner)]

    def r2_copies(c):
        return [remote(p2s.at[c], p2r.at[c], rs.at[2, c], rr.at[2, c], ypeer),
                remote(e2s.at[c], e2r.at[c], rs.at[3, c], rr.at[3, c], ypeer)]

    def r3_copies(c):
        out = []
        for k in (1, 2, 3):
            out.append(remote(p3s.at[c, k - 1], p3r.at[c, k - 1], rs.at[2 + 2 * k, c], rr.at[2 + 2 * k, c], zpeer[k]))
            out.append(remote(e3s.at[c, k - 1], e3r.at[c, k - 1], rs.at[3 + 2 * k, c], rr.at[3 + 2 * k, c], zpeer[k]))
        return out

    def prefetch(c, carry):
        own_q(c).start()
        for cp in kv_copies(c):
            cp.start()
        return carry

    lax.fori_loop(0, nc, prefetch, 0)

    barrier = pltpu.get_barrier_semaphore()
    peers = (partner, ypeer, zpeer[1], zpeer[2], zpeer[3])
    for dev in peers:
        pl.semaphore_signal(barrier, inc=1, device_id={"dup": dev}, device_id_type=MESH)
    pl.semaphore_wait(barrier, len(peers))

    rowid = lax.broadcasted_iota(jnp.int32, (rows, span), 0)
    lane = lax.broadcasted_iota(jnp.int32, (rows, span), 1)
    slot = (rowid * 171) >> 9
    item = rowid - 3 * slot
    rel = (slot & 3) * 4 + ((slot >> 2) & 1) * 2 + (slot >> 3)
    tok = (own * (rel ^ me) + item) & 3
    posm[...] = me * span + lane + 4 - tok
    for ref in (e1s, e2s, e3s, e3k, e1k, e2k):
        ref[...] = jnp.zeros_like(ref)
    wtmp[...] = jnp.zeros_like(wtmp)

    def g1(c):
        for cp in own_sends(c):
            cp.start()

    def g2(c):
        for k in (1, 2, 3):
            wait_slot(c, k)
            for cp in z_forwards(c, k):
                cp.start()

    def g3(c):
        for k in range(4):
            wait_slot(c, 4 + k)
            for cp in y_forwards(c, k):
                cp.start()

    def compute(c):
        for s in range(8, 16):
            wait_slot(c, s)
        own_q(c).wait()
        for s in range(16):
            for i in range(own):
                qf[pl.ds((s * own + i) * pitch, bc), :] = qbuf[c, s, i].astype(F32)
        for cp in kv_copies(c):
            cp.wait()
        base = (c % 2) * (rows * pitch)
        macc[...] = jnp.zeros_like(macc)
        laccs[...] = jnp.ones_like(laccs)
        lanes = lax.broadcasted_iota(jnp.int32, (rows, 128), 1)

        def group(g, carry):
            mv, lv = macc[...], laccs[...]
            for u in range(UNROLL):
                j = g * UNROLL + u
                b = c * bc + j
                qb = qf[pl.ds(j, rows, stride=pitch), :].astype(BF16)
                s = lax.dot_general(qb, kbuf[b], (((1,), (1,)), ((), ())), preferred_element_type=F32)
                s = jnp.where(posm[...] <= len_ref[b], s, NEG)
                mx = jnp.maximum(jnp.max(s, axis=1, keepdims=True), FLOOR)
                p = jnp.exp2((s - mx) * (scale * math.log2(math.e)))
                den = jnp.maximum(jnp.sum(p, axis=1, keepdims=True), 1.0)
                o = jnp.dot(p.astype(BF16), vbuf[b], preferred_element_type=F32) * (1.0 / den)
                of[pl.ds(base + j, rows, stride=pitch), :] = o
                hit = lanes == j
                mv = jnp.where(hit, mx, mv)
                lv = jnp.where(hit, den, lv)
            macc[...] = mv
            laccs[...] = lv
            return carry

        lax.fori_loop(0, bc // UNROLL, group, 0)
        lse = macc[...] * scale + jnp.log(laccs[...])
        e1s[c] = lse[half:]
        e1k[c] = lse[:half]
        for r in range(half):
            p1s[c, r] = of[pl.ds(base + (half + r) * pitch, bc), :].astype(BF16)
        for cp in r1_copies(c):
            cp.start()

    def merge(a, b):
        top = jnp.maximum(a, b)
        ea, eb = jnp.exp(a - top), jnp.exp(b - top)
        tot = ea + eb
        return eb / tot, top + jnp.log(tot)

    def r2(c):
        for cp in r1_copies(c):
            cp.wait_recv()
        base = (c % 2) * (rows * pitch)
        w, lse = merge(e1k[c], e1r[c])
        e2k[c] = lse[:quar]
        e2s[c] = lse[quar:]
        wt = w.T
        for r in list(range(quar, half)) + list(range(quar)):
            wb = wt[:bc, r:r + 1]
            o1 = of[pl.ds(base + r * pitch, bc), :]
            o = (1.0 - wb) * o1 + wb * p1r[c, r].astype(F32)
            if r < quar:
                p2k[c, r] = o
            else:
                p2s[c, r - quar] = o.astype(BF16)
        for cp in r2_copies(c):
            cp.start()

    def r3(c):
        for cp in r2_copies(c):
            cp.wait_recv()
        w, lse = merge(e2k[c], e2r[c])
        for k in range(4):
            if k:
                e3s[c, k - 1, 0:own] = lse[k * own:(k + 1) * own]
            else:
                e3k[c, 0:own] = lse[:own]
        wtmp[0:quar] = w
        wt = wtmp[...].T
        for r in list(range(own, quar)) + list(range(own)):
            wb = wt[:bc, r:r + 1]
            o = (1.0 - wb) * p2k[c, r] + wb * p2r[c, r].astype(F32)
            if r < own:
                p3k[c, r] = o
            else:
                p3s[c, r // own - 1, r % own] = o.astype(BF16)
        for cp in r3_copies(c):
            cp.start()

    def r4(c):
        for cp in r3_copies(c):
            cp.wait_recv()
        ls = [e3k[c]] + [e3r[c, k] for k in range(3)]
        top = jnp.maximum(jnp.maximum(ls[0], ls[1]), jnp.maximum(ls[2], ls[3]))
        es = [jnp.exp(x - top) for x in ls]
        inv = 1.0 / (es[0] + es[1] + es[2] + es[3])
        for k in range(4):
            wtmp[4 * k:4 * k + 4] = es[k] * inv
        wt = wtmp[...].T
        for i in range(own):
            o = wt[:bc, i:i + 1] * p3k[c, i]
            for k in range(3):
                o = o + wt[:bc, 4 * k + 4 + i:4 * k + 5 + i] * p3r[c, k, i].astype(F32)
            out_ref[i, pl.ds(c * bc, bc)] = o.astype(BF16)

    g1(0)
    g1(1)
    g2(0)

    def step(st, carry):
        pl.when(st + 2 < nc)(lambda: g1(st + 2))
        pl.when(st + 1 < nc)(lambda: g2(st + 1))

        @pl.when(st < nc)
        def _():
            g3(st)
            compute(st)

        pl.when((st >= 1) & (st < nc + 1))(lambda: r2(st - 1))
        pl.when((st >= 2) & (st < nc + 2))(lambda: r3(st - 2))
        pl.when(st >= 3)(lambda: r4(st - 3))
        return carry

    lax.fori_loop(0, nc + 3, step, 0)

    def drain(c, carry):
        for cp in own_sends(c):
            cp.wait_send()
        for k in (1, 2, 3):
            for cp in z_forwards(c, k):
                cp.wait_send()
        for k in range(4):
            for cp in y_forwards(c, k):
                cp.wait_send()
        for cp in r1_copies(c) + r2_copies(c) + r3_copies(c):
            cp.wait_send()
        return carry

    lax.fori_loop(0, nc, drain, 0)


def solution(mesh):
    def group_step(q_local, k_span, v_span, len_local):
        nb, own, dim = q_local.shape
        span = k_span.shape[1]
        rows = 16 * own
        half, quar = rows // 2, rows // 4
        nc = CHUNKS
        bc = nb // nc
        pitch = bc + 8
        q_planes = jnp.transpose(q_local, (1, 0, 2))
        vm = pltpu.VMEM
        dma = pltpu.SemaphoreType.DMA
        any_spec = pl.BlockSpec(memory_space=pl.ANY)
        out = pl.pallas_call(
            functools.partial(fused, nb, own, span, dim),
            out_shape=jax.ShapeDtypeStruct((own, nb, dim), BF16),
            in_specs=[pl.BlockSpec(memory_space=pltpu.SMEM), any_spec, any_spec, any_spec],
            out_specs=pl.BlockSpec(memory_space=vm),
            scratch_shapes=[
                vm((nb, span, dim), BF16), vm((nb, span, dim), BF16),
                vm((nc, 16, own, bc, dim), BF16),
                vm((rows * pitch, dim), F32), vm((2 * rows * pitch, dim), F32),
                vm((rows, span), jnp.int32), vm((rows, 128), F32), vm((rows, 128), F32),
                vm((nc, half, bc, dim), BF16), vm((nc, half, bc, dim), BF16),
                vm((nc, half, 128), F32), vm((nc, half, 128), F32), vm((nc, half, 128), F32),
                vm((nc, quar, bc, dim), BF16), vm((nc, quar, bc, dim), F32), vm((nc, quar, bc, dim), BF16),
                vm((nc, quar, 128), F32), vm((nc, quar, 128), F32), vm((nc, quar, 128), F32),
                vm((nc, 3, own, bc, dim), BF16), vm((nc, own, bc, dim), F32), vm((nc, 3, own, bc, dim), BF16),
                vm((nc, 3, 4, 128), F32), vm((nc, 4, 128), F32), vm((nc, 3, 4, 128), F32),
                vm((16, 128), F32),
                dma((2, nc)), dma((nc,)), dma((16, nc)), dma((16, nc)), dma((10, nc)), dma((10, nc)),
            ],
            compiler_params=pltpu.CompilerParams(
                collective_id=0, has_side_effects=True, vmem_limit_bytes=67043328),
            name="attend",
        )(len_local, q_planes, k_span, v_span)
        return jnp.transpose(out, (1, 0, 2))

    return jax.shard_map(group_step, mesh=mesh, in_specs=(P("kv", "dup", None), P("kv", "dup", None), P("kv", "dup", None), P("kv")), out_specs=P("kv", "dup", None), check_vma=False)
```

```python
import functools
import math

import jax
import jax.numpy as jnp
from jax import lax
from jax.experimental import pallas as pl
from jax.experimental.pallas import tpu as pltpu
from jax.sharding import PartitionSpec as P

DRAFT = 4
CHUNKS = 8
UNROLL = 8
NEG = -3.4e38
FLOOR = -3.0e38
MESH = pl.DeviceIdType.MESH
F32 = jnp.float32
BF16 = jnp.bfloat16


def fused(nb, own, span, dim, len_ref, q_ref, k_ref, v_ref, out_ref,
          kbuf, vbuf, qbuf, qf, of, posm, macc, laccs, sbuf, pbuf,
          p1s, p1r, e1s, e1k, e1r, p2s, p2k, p2r, e2s, e2k, e2r, p3s, p3k, p3r, e3s, e3k, e3r,
          wtmp, kvsem, qsem, gs, gr, rs, rr):
    nc = CHUNKS
    bc = nb // nc
    pitch = bc + 8
    rows = 16 * own
    half, quar = rows // 2, rows // 4
    scale = dim ** -0.5
    me = lax.axis_index("dup")
    core, yy, zz = me % 2, (me // 2) % 2, me // 4
    partner = me + 1 - 2 * core
    ypeer = me + 2 - 4 * yy
    zpeer = [None,
             me + 4 * (1 - 2 * (zz % 2)),
             me + 4 * (2 - 4 * (zz // 2)),
             me + 4 * (3 - 2 * zz)]

    def kv_copies(c):
        sl = pl.ds(c * bc, bc)
        return (pltpu.make_async_copy(k_ref.at[sl], kbuf.at[sl], kvsem.at[0, c]),
                pltpu.make_async_copy(v_ref.at[sl], vbuf.at[sl], kvsem.at[1, c]))

    def own_q(c):
        return pltpu.make_async_copy(q_ref.at[:, pl.ds(c * bc, bc)], qbuf.at[c, 0], qsem.at[c])

    def remote(src, dst, ssem, rsem, dev):
        return pltpu.make_async_remote_copy(src_ref=src, dst_ref=dst, send_sem=ssem, recv_sem=rsem,
                                            device_id={"dup": dev}, device_id_type=MESH)

    def send_own(c, slot, dev, idx):
        return remote(q_ref.at[:, pl.ds(c * bc, bc)], qbuf.at[c, slot], gs.at[idx, c], gr.at[slot, c], dev)

    def forward(c, slot_from, slot_to, dev, idx):
        return remote(qbuf.at[c, slot_from], qbuf.at[c, slot_to], gs.at[idx, c], gr.at[slot_to, c], dev)

    def own_sends(c):
        return ([send_own(c, k, zpeer[k], k) for k in (1, 2, 3)]
                + [send_own(c, 4, ypeer, 4), send_own(c, 8, partner, 8)])

    def z_forwards(c, k):
        return [forward(c, k, 4 + k, ypeer, 4 + k), forward(c, k, 8 + k, partner, 8 + k)]

    def y_forwards(c, k):
        return [forward(c, 4 + k, 12 + k, partner, 12 + k)]

    def wait_slot(c, slot):
        forward(c, slot, slot, partner, 0).wait_recv()

    def r1_copies(c):
        return [remote(p1s.at[c], p1r.at[c], rs.at[0, c], rr.at[0, c], partner),
                remote(e1s.at[c], e1r.at[c], rs.at[1, c], rr.at[1, c], partner)]

    def r2_copies(c):
        return [remote(p2s.at[c], p2r.at[c], rs.at[2, c], rr.at[2, c], ypeer),
                remote(e2s.at[c], e2r.at[c], rs.at[3, c], rr.at[3, c], ypeer)]

    def r3_copies(c):
        out = []
        for k in (1, 2, 3):
            out.append(remote(p3s.at[c, k - 1], p3r.at[c, k - 1], rs.at[2 + 2 * k, c], rr.at[2 + 2 * k, c], zpeer[k]))
            out.append(remote(e3s.at[c, k - 1], e3r.at[c, k - 1], rs.at[3 + 2 * k, c], rr.at[3 + 2 * k, c], zpeer[k]))
        return out

    def prefetch(c, carry):
        own_q(c).start()
        for cp in kv_copies(c):
            cp.start()
        return carry

    lax.fori_loop(0, nc, prefetch, 0)

    barrier = pltpu.get_barrier_semaphore()
    peers = (partner, ypeer, zpeer[1], zpeer[2], zpeer[3])
    for dev in peers:
        pl.semaphore_signal(barrier, inc=1, device_id={"dup": dev}, device_id_type=MESH)
    pl.semaphore_wait(barrier, len(peers))

    rowid = lax.broadcasted_iota(jnp.int32, (rows, span), 0)
    lane = lax.broadcasted_iota(jnp.int32, (rows, span), 1)
    slot = (rowid * 171) >> 9
    item = rowid - 3 * slot
    rel = (slot & 3) * 4 + ((slot >> 2) & 1) * 2 + (slot >> 3)
    tok = (own * (rel ^ me) + item) & 3
    posm[...] = me * span + lane + 4 - tok
    for ref in (e1s, e2s, e3s, e3k, e1k, e2k):
        ref[...] = jnp.zeros_like(ref)
    wtmp[...] = jnp.zeros_like(wtmp)

    def g1(c):
        for cp in own_sends(c):
            cp.start()

    def g2(c):
        for k in (1, 2, 3):
            wait_slot(c, k)
            for cp in z_forwards(c, k):
                cp.start()

    def g3(c):
        for k in range(4):
            wait_slot(c, 4 + k)
            for cp in y_forwards(c, k):
                cp.start()

    def compute(c):
        for s in range(8, 16):
            wait_slot(c, s)
        own_q(c).wait()
        for s in range(16):
            for i in range(own):
                qf[pl.ds((s * own + i) * pitch, bc), :] = qbuf[c, s, i].astype(F32)
        for cp in kv_copies(c):
            cp.wait()
        base = (c % 2) * (rows * pitch)
        macc[...] = jnp.zeros_like(macc)
        laccs[...] = jnp.ones_like(laccs)
        lanes = lax.broadcasted_iota(jnp.int32, (rows, 128), 1)

        def scores(j):
            qb = qf[pl.ds(j, rows, stride=pitch), :].astype(BF16)
            sbuf[j] = lax.dot_general(qb, kbuf[c * bc + j], (((1,), (1,)), ((), ())), preferred_element_type=F32)

        def soften(j, mv, lv):
            s = jnp.where(posm[...] <= len_ref[c * bc + j], sbuf[j], NEG)
            mx = jnp.maximum(jnp.max(s, axis=1, keepdims=True), FLOOR)
            p = jnp.exp2((s - mx) * (scale * math.log2(math.e)))
            pbuf[j] = p.astype(BF16)
            hit = lanes == j
            return jnp.where(hit, mx, mv), jnp.where(hit, jnp.sum(p, axis=1, keepdims=True), lv)

        def weigh(j):
            of[pl.ds(base + j, rows, stride=pitch), :] = jnp.dot(pbuf[j], vbuf[c * bc + j], preferred_element_type=F32)

        def soften_group(g, carry):
            mv, lv = macc[...], laccs[...]
            for u in range(UNROLL):
                mv, lv = soften(g * UNROLL + u, mv, lv)
            macc[...] = mv
            laccs[...] = lv
            return carry

        for j in range(bc):
            scores(j)
        lax.fori_loop(0, bc // UNROLL, soften_group, 0)
        for j in range(bc):
            weigh(j)
        mx, den = macc[...] * scale, laccs[...]
        e1k[c, 0], e1k[c, 1] = mx[:half], den[:half]
        e1s[c, 0], e1s[c, 1] = mx[half:], den[half:]
        for r in range(half):
            p1s[c, r] = of[pl.ds(base + (half + r) * pitch, bc), :].astype(BF16)
        for cp in r1_copies(c):
            cp.start()

    def merge(a, b):
        top = jnp.maximum(a, b)
        ea, eb = jnp.exp(a - top), jnp.exp(b - top)
        tot = ea + eb
        return eb / tot, top + jnp.log(tot)

    def r2(c):
        for cp in r1_copies(c):
            cp.wait_recv()
        base = (c % 2) * (rows * pitch)
        ma, mb = e1k[c, 0], e1r[c, 0]
        top = jnp.maximum(ma, mb)
        ea, eb = jnp.exp(ma - top), jnp.exp(mb - top)
        tot = jnp.maximum(ea * e1k[c, 1] + eb * e1r[c, 1], 1.0)
        lse = top + jnp.log(tot)
        inv = 1.0 / tot
        e2k[c] = lse[:quar]
        e2s[c] = lse[quar:]
        wat, wbt = (ea * inv).T, (eb * inv).T
        for r in list(range(quar, half)) + list(range(quar)):
            o = (wat[:bc, r:r + 1] * of[pl.ds(base + r * pitch, bc), :]
                 + wbt[:bc, r:r + 1] * p1r[c, r].astype(F32))
            if r < quar:
                p2k[c, r] = o
            else:
                p2s[c, r - quar] = o.astype(BF16)
        for cp in r2_copies(c):
            cp.start()

    def r3(c):
        for cp in r2_copies(c):
            cp.wait_recv()
        w, lse = merge(e2k[c], e2r[c])
        for k in range(4):
            if k:
                e3s[c, k - 1, 0:own] = lse[k * own:(k + 1) * own]
            else:
                e3k[c, 0:own] = lse[:own]
        wtmp[0:quar] = w
        wt = wtmp[...].T
        for r in list(range(own, quar)) + list(range(own)):
            wb = wt[:bc, r:r + 1]
            o = (1.0 - wb) * p2k[c, r] + wb * p2r[c, r].astype(F32)
            if r < own:
                p3k[c, r] = o
            else:
                p3s[c, r // own - 1, r % own] = o.astype(BF16)
        for cp in r3_copies(c):
            cp.start()

    def r4(c):
        for cp in r3_copies(c):
            cp.wait_recv()
        ls = [e3k[c]] + [e3r[c, k] for k in range(3)]
        top = jnp.maximum(jnp.maximum(ls[0], ls[1]), jnp.maximum(ls[2], ls[3]))
        es = [jnp.exp(x - top) for x in ls]
        inv = 1.0 / (es[0] + es[1] + es[2] + es[3])
        for k in range(4):
            wtmp[4 * k:4 * k + 4] = es[k] * inv
        wt = wtmp[...].T
        for i in range(own):
            o = wt[:bc, i:i + 1] * p3k[c, i]
            for k in range(3):
                o = o + wt[:bc, 4 * k + 4 + i:4 * k + 5 + i] * p3r[c, k, i].astype(F32)
            out_ref[i, pl.ds(c * bc, bc)] = o.astype(BF16)

    g1(0)
    g1(1)
    g2(0)

    def step(st, carry):
        pl.when(st + 2 < nc)(lambda: g1(st + 2))
        pl.when(st + 1 < nc)(lambda: g2(st + 1))

        @pl.when(st < nc)
        def _():
            g3(st)
            compute(st)

        pl.when((st >= 1) & (st < nc + 1))(lambda: r2(st - 1))
        pl.when((st >= 2) & (st < nc + 2))(lambda: r3(st - 2))
        pl.when(st >= 3)(lambda: r4(st - 3))
        return carry

    lax.fori_loop(0, nc + 3, step, 0)

    def drain(c, carry):
        for cp in own_sends(c):
            cp.wait_send()
        for k in (1, 2, 3):
            for cp in z_forwards(c, k):
                cp.wait_send()
        for k in range(4):
            for cp in y_forwards(c, k):
                cp.wait_send()
        for cp in r1_copies(c) + r2_copies(c) + r3_copies(c):
            cp.wait_send()
        return carry

    lax.fori_loop(0, nc, drain, 0)


def solution(mesh):
    def group_step(q_local, k_span, v_span, len_local):
        nb, own, dim = q_local.shape
        span = k_span.shape[1]
        rows = 16 * own
        half, quar = rows // 2, rows // 4
        nc = CHUNKS
        bc = nb // nc
        pitch = bc + 8
        q_planes = jnp.transpose(q_local, (1, 0, 2))
        vm = pltpu.VMEM
        dma = pltpu.SemaphoreType.DMA
        any_spec = pl.BlockSpec(memory_space=pl.ANY)
        out = pl.pallas_call(
            functools.partial(fused, nb, own, span, dim),
            out_shape=jax.ShapeDtypeStruct((own, nb, dim), BF16),
            in_specs=[pl.BlockSpec(memory_space=pltpu.SMEM), any_spec, any_spec, any_spec],
            out_specs=pl.BlockSpec(memory_space=vm),
            scratch_shapes=[
                vm((nb, span, dim), BF16), vm((nb, span, dim), BF16),
                vm((nc, 16, own, bc, dim), BF16),
                vm((rows * pitch, dim), F32), vm((2 * rows * pitch, dim), F32),
                vm((rows, span), jnp.int32), vm((rows, 128), F32), vm((rows, 128), F32), vm((bc, rows, span), F32), vm((bc, rows, span), BF16),
                vm((nc, half, bc, dim), BF16), vm((nc, half, bc, dim), BF16),
                vm((nc, 2, half, 128), F32), vm((nc, 2, half, 128), F32), vm((nc, 2, half, 128), F32),
                vm((nc, quar, bc, dim), BF16), vm((nc, quar, bc, dim), F32), vm((nc, quar, bc, dim), BF16),
                vm((nc, quar, 128), F32), vm((nc, quar, 128), F32), vm((nc, quar, 128), F32),
                vm((nc, 3, own, bc, dim), BF16), vm((nc, own, bc, dim), F32), vm((nc, 3, own, bc, dim), BF16),
                vm((nc, 3, 4, 128), F32), vm((nc, 4, 128), F32), vm((nc, 3, 4, 128), F32),
                vm((16, 128), F32),
                dma((2, nc)), dma((nc,)), dma((16, nc)), dma((16, nc)), dma((10, nc)), dma((10, nc)),
            ],
            compiler_params=pltpu.CompilerParams(
                collective_id=0, has_side_effects=True, vmem_limit_bytes=67043328),
            name="attend",
        )(len_local, q_planes, k_span, v_span)
        return jnp.transpose(out, (1, 0, 2))

    return jax.shard_map(group_step, mesh=mesh, in_specs=(P("kv", "dup", None), P("kv", "dup", None), P("kv", "dup", None), P("kv")), out_specs=P("kv", "dup", None), check_vma=False)
```

```python
import functools
import math

import jax
import jax.numpy as jnp
from jax import lax
from jax.experimental import pallas as pl
from jax.experimental.pallas import tpu as pltpu
from jax.sharding import PartitionSpec as P

CHUNKS = 8
UNROLL = 32
AHEAD = 3
LAG = (0, 1, 3, 4, 5, 7, 9, 11)
B_MOD, B_REM = 100, 50
NEG = -3.4e38
FLOOR = -3.0e38
MESH = pl.DeviceIdType.MESH
F32 = jnp.float32
BF16 = jnp.bfloat16
N_B = len([c for c in range(CHUNKS) if c % B_MOD == B_REM])
N_A = CHUNKS - N_B


def fused(nb, own, span, dim, len_ref, q_ref, k_ref, v_ref, out_ref,
          kbuf, vbuf, qbuf, qf, of, posm, macc, dacc, sbuf, pbuf,
          p1s, p1r, e1k, e1s, e1r, part, lse, ltmp,
          ys, yr, zns, znr, zos, zor, zfs, zfr,
          eys, eyr, ens, enr, eos, eor, efs, efr,
          kvsem, qsem, ss, rq, rr):
    nc = CHUNKS
    bc = nb // nc
    pitch = bc + 8
    rows = 16 * own
    half = rows // 2
    scale = dim ** -0.5
    me = lax.axis_index("dup")
    core, yy, zz = me % 2, (me // 2) % 2, me // 4
    inner = ((zz + 1) // 2) % 2
    partner = me + 1 - 2 * core
    ypeer = me + 2 - 4 * yy
    z1 = me + 4 * (1 - 2 * (zz % 2))
    z2 = me + 4 * (2 - 4 * (zz // 2))
    z3 = me + 4 * (3 - 2 * zz)
    far_inner = me + 4 * (2 - zz // 2 - zz)

    def is_b(c):
        return c % B_MOD == B_REM

    def by_type(c, fn):
        pl.when(is_b(c))(lambda: fn(c, 2))
        pl.when(jnp.logical_not(is_b(c)))(lambda: fn(c, 1))

    def remote(src, dst, ssem, rsem, dev):
        return pltpu.make_async_remote_copy(src_ref=src, dst_ref=dst, send_sem=ssem, recv_sem=rsem,
                                            device_id={"dup": dev}, device_id_type=MESH)

    def send(src, dst, si, rsem, dev):
        remote(src, dst, ss.at[si], rsem, dev).start()

    def recv(ref, rsem):
        remote(ref, ref, ss.at[0], rsem, partner).wait_recv()

    def kv_copies(c):
        sl = pl.ds(c * bc, bc)
        return (pltpu.make_async_copy(k_ref.at[sl], kbuf.at[sl], kvsem.at[c]),
                pltpu.make_async_copy(v_ref.at[sl], vbuf.at[sl], kvsem.at[c]))

    def own_q(c):
        return pltpu.make_async_copy(q_ref.at[:, pl.ds(c * bc, bc)], qbuf.at[c, 0, 0, 0], qsem)

    def start_q(c, carry):
        own_q(c).start()
        return carry

    def start_kv(c, carry):
        for cp in kv_copies(c):
            cp.start()
        return carry

    lax.fori_loop(0, nc, start_q, 0)
    lax.fori_loop(0, nc, start_kv, 0)

    barrier = pltpu.get_barrier_semaphore()
    peers = (partner, ypeer, z1, z2, z3)
    for dev in peers:
        pl.semaphore_signal(barrier, inc=1, device_id={"dup": dev}, device_id_type=MESH)

    rowid = lax.broadcasted_iota(jnp.int32, (rows, span), 0)
    lane = lax.broadcasted_iota(jnp.int32, (rows, span), 1)
    slot = (rowid * 171) >> 9
    item = rowid - 3 * slot
    rel = (slot & 3) * 4 + ((slot >> 2) & 1) * 2 + (slot >> 3)
    tok = (own * (rel ^ me) + item) & 3
    posm[...] = me * span + lane + 4 - tok
    ltmp[...] = jnp.zeros_like(ltmp)

    pltpu.make_async_copy(q_ref, q_ref, qsem).wait()
    pl.semaphore_wait(barrier, len(peers))

    def q_z_own(c, ny):
        y = pl.ds(0, ny)
        src = qbuf.at[c, 0, y, 0]
        send(src, qbuf.at[c, 0, y, 2 + inner], ny - 1, rq.at[1, c], far_inner)
        send(src, qbuf.at[c, 0, y, 1], ny - 1, rq.at[0, c], z1)

    def q_z_relay(c, ny):
        y = pl.ds(0, ny)
        recv(qbuf.at[c, 0, y, pl.ds(2, 2)], rq.at[1, c])

        @pl.when(inner == 1)
        def _():
            send(qbuf.at[c, 0, y, 2], qbuf.at[c, 0, y, 3], 2 + ny - 1, rq.at[1, c], z1)
            send(qbuf.at[c, 0, y, 3], qbuf.at[c, 0, y, 2], 2 + ny - 1, rq.at[1, c], z1)

    def q_z_end(c, ny):
        recv(qbuf.at[c, 0, pl.ds(0, ny), 1], rq.at[0, c])

    def q_y(c, ny):
        if ny == 1:
            z = pl.ds(1, 3)
            send(qbuf.at[c, 0, 0, z], qbuf.at[c, 0, 1, z], 4, rq.at[2, c], ypeer)
        else:
            send(qbuf.at[c, 0, 0, 0], qbuf.at[c, 0, 1, 0], 5, rq.at[2, c], ypeer)

    def q_y_wait(c, ny):
        recv(qbuf.at[c, 0, 1] if ny == 1 else qbuf.at[c, 0, 1, 0], rq.at[2, c])

    def q0(c, ny):
        if ny == 1:
            q_z_own(c, ny)
            send(qbuf.at[c, 0, 0, 0], qbuf.at[c, 0, 1, 0], 4, rq.at[2, c], ypeer)
        else:
            q_y(c, ny)

    def q1(c, ny):
        if ny == 1:
            pl.when(inner == 1)(lambda: q_z_relay(c, ny))
        else:
            q_y_wait(c, ny)
            q_z_own(c, ny)

    def q2(c, ny):
        if ny == 1:
            q_z_end(c, ny)
            pl.when(inner == 0)(lambda: q_z_relay(c, ny))
            q_y(c, ny)
        else:
            pl.when(inner == 1)(lambda: q_z_relay(c, ny))

    def q3(c, ny):
        if ny == 1:
            q_y_wait(c, ny)
        else:
            q_z_end(c, ny)
            pl.when(inner == 0)(lambda: q_z_relay(c, ny))

    def q_partner(c):
        send(qbuf.at[c, 0], qbuf.at[c, 1], 6, rq.at[3, c], partner)

    def compute(c):
        recv(qbuf.at[c, 1], rq.at[3, c])
        for s in range(16):
            for i in range(own):
                qf[pl.ds((s * own + i) * pitch, bc), :] = qbuf[c, s // 8, (s // 4) % 2, s % 4, i].astype(F32)
        pltpu.make_async_copy(k_ref.at[pl.ds(0, 2 * bc)], kbuf.at[pl.ds(0, 2 * bc)], kvsem.at[c]).wait()
        base = (c % 2) * (rows * pitch)
        macc[...] = jnp.zeros_like(macc)
        dacc[...] = jnp.zeros_like(dacc)
        place = lax.broadcasted_iota(jnp.int32, (rows, 128), 1)
        rid = lax.broadcasted_iota(jnp.int32, (rows, 128), 0)
        place = place - bc * (rid - 3 * ((rid * 171) >> 9))

        def scores(j):
            qb = qf[pl.ds(j, rows, stride=pitch), :].astype(BF16)
            sbuf[j] = lax.dot_general(qb, kbuf[c * bc + j], (((1,), (1,)), ((), ())), preferred_element_type=F32)

        def soften(j, mv, dv):
            s = jnp.where(posm[...] <= len_ref[c * bc + j], sbuf[j], NEG)
            mx = jnp.maximum(jnp.max(s, axis=1, keepdims=True), FLOOR)
            p = jnp.exp2((s - mx) * (scale * math.log2(math.e)))
            pbuf[j] = p.astype(BF16)
            hit = place == j
            return jnp.where(hit, mx, mv), jnp.where(hit, jnp.sum(p, axis=1, keepdims=True), dv)

        def soften_group(g, carry):
            mv, dv = macc[...], dacc[...]
            for u in range(UNROLL):
                mv, dv = soften(g * UNROLL + u, mv, dv)
            macc[...] = mv
            dacc[...] = dv
            return carry

        for j in range(bc):
            scores(j)
        lax.fori_loop(0, bc // UNROLL, soften_group, 0)
        for j in range(bc):
            of[pl.ds(base + j, rows, stride=pitch), :] = jnp.dot(pbuf[j], vbuf[c * bc + j], preferred_element_type=F32)
        for t, acc in ((0, macc), (1, dacc)):
            line = acc[pl.ds(0, 16, stride=3), :] + acc[pl.ds(1, 16, stride=3), :] + acc[pl.ds(2, 16, stride=3), :]
            if t == 0:
                line = line * scale
            e1k[c, t] = line[:8]
            e1s[c, t] = line[8:]
        for r in range(half):
            p1s[c, r] = of[pl.ds(base + (half + r) * pitch, bc), :].astype(BF16)
        send(e1s.at[c], e1r.at[c], 8, rr.at[1, c], partner)
        send(p1s.at[c], p1r.at[c], 7, rr.at[0, c], partner)

    def cut(w, line, i):
        return w[i * bc:(i + 1) * bc, line:line + 1]

    def lines(refs):
        for n, ref in refs:
            ltmp[n:n + 1] = ref
        return ltmp[...]

    def weights(*ls):
        top = functools.reduce(jnp.maximum, ls)
        es = [jnp.exp(x - top) for x in ls]
        tot = functools.reduce(lambda a, b: a + b, es)
        inv = 1.0 / tot
        return [(e * inv).T for e in es], top + jnp.log(tot)

    def merge_partner(c):
        recv(e1r.at[c], rr.at[1, c])
        ma, mb = e1k[c, 0], e1r[c, 0]
        top = jnp.maximum(ma, mb)
        ea, eb = jnp.exp(ma - top), jnp.exp(mb - top)
        tot = jnp.maximum(ea * e1k[c, 1] + eb * e1r[c, 1], 1.0)
        inv = 1.0 / tot
        lse[c] = top + jnp.log(tot)
        wa, wb = (ea * inv).T, (eb * inv).T
        recv(p1r.at[c], rr.at[0, c])
        base = (c % 2) * (rows * pitch)
        for n in range(8):
            for i in range(own):
                r = n * own + i
                part[c, n, i] = (cut(wa, n, i) * of[pl.ds(base + r * pitch, bc), :]
                                 + cut(wb, n, i) * p1r[c, r].astype(F32))

    def y_send(c, ny):
        for z in range(4 if ny == 1 else 1):
            eys[c, z] = lse[c, 4 + z:5 + z]
            for i in range(own):
                ys[c, z, i] = part[c, 4 + z, i].astype(BF16)
        if ny == 1:
            send(eys.at[c], eyr.at[c], 10, rr.at[3, c], ypeer)
            send(ys.at[c], yr.at[c], 9, rr.at[2, c], ypeer)
        else:
            send(eys.at[c, 0], eyr.at[c, 0], 12, rr.at[3, c], ypeer)
            send(ys.at[c, 0], yr.at[c, 0], 11, rr.at[2, c], ypeer)

    def y_merge(c, ny):
        if ny == 1:
            recv(eyr.at[c], rr.at[3, c])
            (wa, wb), new = weights(lse[c], lines([(z, eyr[c, z]) for z in range(4)]))
            lse[c] = new
            recv(yr.at[c], rr.at[2, c])
            for z in range(4):
                for i in range(own):
                    part[c, z, i] = cut(wa, z, i) * part[c, z, i] + cut(wb, z, i) * yr[c, z, i].astype(F32)
        else:
            recv(eyr.at[c, 0], rr.at[3, c])
            (wa, wb), _ = weights(lse[c], lines([(0, eyr[c, 0])]))
            recv(yr.at[c, 0], rr.at[2, c])
            for i in range(own):
                o = cut(wa, 0, i) * part[c, 0, i] + cut(wb, 0, i) * yr[c, 0, i].astype(F32)
                out_ref[i, pl.ds(c * bc, bc)] = o.astype(BF16)

    def z_send(c, ny):
        y = pl.ds(0, ny)

        @pl.when(inner == 0)
        def _():
            for m in range(2):
                for h in range(ny):
                    eos[c, m, h] = lse[c, 4 * h + 2 + m:4 * h + 3 + m]
                    for i in range(own):
                        zos[c, m, h, i] = part[c, 4 * h + 2 + m, i].astype(BF16)
            send(eos.at[c, :, y], eor.at[c, :, y], 18 + 2 * (ny - 1), rr.at[7, c], z1)
            send(zos.at[c, :, y], zor.at[c, :, y], 17 + 2 * (ny - 1), rr.at[6, c], z1)

        for h in range(ny):
            ens[c, h] = lse[c, 4 * h + 1:4 * h + 2]
            for i in range(own):
                zns[c, h, i] = part[c, 4 * h + 1, i].astype(BF16)
        send(ens.at[c, y], enr.at[c, y], 14 + 2 * (ny - 1), rr.at[5, c], z1)
        send(zns.at[c, y], znr.at[c, y], 13 + 2 * (ny - 1), rr.at[4, c], z1)

    def z_relay(c, ny):
        y = pl.ds(0, ny)
        recv(eor.at[c, :, y], rr.at[7, c])
        (wa, wb), new = weights(lse[c], lines([(4 * h + 3 - m, eor[c, m, h]) for m in range(2) for h in range(ny)]))
        recv(zor.at[c, :, y], rr.at[6, c])
        for m in range(2):
            for h in range(ny):
                n = 4 * h + 3 - m
                efs[c, m, h] = new[n:n + 1]
                for i in range(own):
                    o = cut(wa, n, i) * part[c, n, i] + cut(wb, n, i) * zor[c, m, h, i].astype(F32)
                    zfs[c, m, h, i] = o.astype(BF16)
        for m, dev in ((1, z2), (0, z3)):
            send(efs.at[c, m, y], efr.at[c, y], 22 + 2 * (ny - 1), rr.at[9, c], dev)
            send(zfs.at[c, m, y], zfr.at[c, y], 21 + 2 * (ny - 1), rr.at[8, c], dev)

    def z_merge(c, ny):
        y = pl.ds(0, ny)
        recv(enr.at[c, y], rr.at[5, c])
        recv(efr.at[c, y], rr.at[9, c])
        near = lines([(4 * h, enr[c, h]) for h in range(ny)])
        far = lines([(4 * h, efr[c, h]) for h in range(ny)])
        (wa, wb, wc), new = weights(lse[c], near, far)
        lse[c] = new
        recv(znr.at[c, y], rr.at[4, c])
        recv(zfr.at[c, y], rr.at[8, c])
        for h in range(ny):
            n = 4 * h
            for i in range(own):
                o = (cut(wa, n, i) * part[c, n, i] + cut(wb, n, i) * znr[c, h, i].astype(F32)
                     + cut(wc, n, i) * zfr[c, h, i].astype(F32))
                if ny == 1:
                    out_ref[i, pl.ds(c * bc, bc)] = o.astype(BF16)
                else:
                    part[c, n, i] = o

    def r0(c):
        merge_partner(c)
        by_type(c, lambda c, ny: y_send(c, ny) if ny == 1 else z_send(c, ny))

    def r1(c, ny):
        if ny == 1:
            y_merge(c, ny)
            z_send(c, ny)
        else:
            pl.when(inner == 1)(lambda: z_relay(c, ny))

    def r2(c, ny):
        if ny == 1:
            pl.when(inner == 1)(lambda: z_relay(c, ny))
        else:
            z_merge(c, ny)
            y_send(c, ny)

    def r3(c, ny):
        if ny == 1:
            z_merge(c, ny)
        else:
            y_merge(c, ny)

    def at(c, fn):
        pl.when((c >= 0) & (c < nc))(lambda: fn(c))

    def typed(fn):
        return lambda c: by_type(c, fn)

    def first(c, carry):
        by_type(c, q0)
        return carry

    lax.fori_loop(0, AHEAD, first, 0)

    def step(st, carry):
        at(st + AHEAD, typed(q0))
        at(st - LAG[0], typed(q1))
        at(st - LAG[1], typed(q2))

        @pl.when((st >= LAG[2]) & (st - LAG[2] < nc))
        def _():
            by_type(st - LAG[2], q3)
            q_partner(st - LAG[2])

        at(st - LAG[3], compute)
        at(st - LAG[4], r0)
        at(st - LAG[5], typed(r1))
        at(st - LAG[6], typed(r2))
        at(st - LAG[7], typed(r3))
        return carry

    lax.fori_loop(0, nc + LAG[7], step, 0)

    def sent(ref, si):
        remote(ref, ref, ss.at[si], rq.at[0, 0], partner).wait_send()

    for t, n in ((0, N_A), (1, N_B)):
        if n == 0:
            continue
        c, y = pl.ds(0, n), pl.ds(0, t + 1)
        sent(qbuf.at[c, 0, y, pl.ds(0, 2)], t)
        sent(qbuf.at[c, 0, 0] if t == 0 else qbuf.at[c, 0, 0, 0], 4 + t)
        sent(ys.at[c] if t == 0 else ys.at[c, 0], 9 + 2 * t)
        sent(eys.at[c] if t == 0 else eys.at[c, 0], 10 + 2 * t)
        sent(zns.at[c, y], 13 + 2 * t)
        sent(ens.at[c, y], 14 + 2 * t)

        @pl.when(inner == 0)
        def _():
            sent(zos.at[c, :, y], 17 + 2 * t)
            sent(eos.at[c, :, y], 18 + 2 * t)

        @pl.when(inner == 1)
        def _():
            sent(qbuf.at[c, 0, y, pl.ds(0, 2)], 2 + t)
            sent(zfs.at[c, :, y], 21 + 2 * t)
            sent(efs.at[c, :, y], 22 + 2 * t)

    sent(qbuf.at[:, 0], 6)
    sent(p1s, 7)
    sent(e1s, 8)


def solution(mesh):
    def group_step(q_local, k_span, v_span, len_local):
        nb, own, dim = q_local.shape
        span = k_span.shape[1]
        rows = 16 * own
        half = rows // 2
        nc = CHUNKS
        bc = nb // nc
        pitch = bc + 8
        q_planes = jnp.transpose(q_local, (1, 0, 2))
        vm = pltpu.VMEM
        dma = pltpu.SemaphoreType.DMA
        any_spec = pl.BlockSpec(memory_space=pl.ANY)

        def blocks(*lead):
            return vm((nc, *lead, own, bc, dim), BF16)

        def line(*lead):
            return vm((nc, *lead, 1, 128), F32)

        out = pl.pallas_call(
            functools.partial(fused, nb, own, span, dim),
            out_shape=jax.ShapeDtypeStruct((own, nb, dim), BF16),
            in_specs=[pl.BlockSpec(memory_space=pltpu.SMEM), any_spec, any_spec, any_spec],
            out_specs=pl.BlockSpec(memory_space=vm),
            scratch_shapes=[
                vm((nb, span, dim), BF16), vm((nb, span, dim), BF16),
                blocks(2, 2, 4),
                vm((rows * pitch, dim), F32), vm((2 * rows * pitch, dim), F32),
                vm((rows, span), jnp.int32), vm((rows, 128), F32), vm((rows, 128), F32),
                vm((bc, rows, span), F32), vm((bc, rows, span), BF16),
                vm((nc, half, bc, dim), BF16), vm((nc, half, bc, dim), BF16),
                vm((nc, 2, 8, 128), F32), vm((nc, 2, 8, 128), F32), vm((nc, 2, 8, 128), F32),
                vm((nc, 8, own, bc, dim), F32), vm((nc, 8, 128), F32), vm((8, 128), F32),
                blocks(4), blocks(4), blocks(2), blocks(2),
                blocks(2, 2), blocks(2, 2), blocks(2, 2), blocks(2),
                line(4), line(4), line(2), line(2), line(2, 2), line(2, 2), line(2, 2), line(2),
                dma((nc,)), dma, dma((25,)), dma((4, nc)), dma((10, nc)),
            ],
            compiler_params=pltpu.CompilerParams(
                collective_id=0, has_side_effects=True, vmem_limit_bytes=67043328),
            name="attend",
        )(len_local, q_planes, k_span, v_span)
        return jnp.transpose(out, (1, 0, 2))

    return jax.shard_map(group_step, mesh=mesh, in_specs=(P("kv", "dup", None), P("kv", "dup", None), P("kv", "dup", None), P("kv")), out_specs=P("kv", "dup", None), check_vma=False)
```

```python
import functools
import math

import jax
import jax.numpy as jnp
from jax import lax
from jax.experimental import pallas as pl
from jax.experimental.pallas import tpu as pltpu
from jax.sharding import PartitionSpec as P

CHUNKS = 8
UNROLL = 32
AHEAD = 2
Y_AHEAD = 3
LAG = (0, 1, 3, 4, 5, 7, 9, 11)
Q_WAY = "AAABAABA"
O_WAY = "DDBDDDDD"
NEG = -3.4e38
FLOOR = -3.0e38
MESH = pl.DeviceIdType.MESH
F32 = jnp.float32
BF16 = jnp.bfloat16
def fused(nb, own, span, dim, len_ref, q_ref, k_ref, v_ref, out_ref,
          kbuf, vbuf, qbuf, qf, of, posm, macc, dacc, sbuf, pbuf,
          p1s, p1r, e1k, e1s, e1r, part, lse, ltmp,
          ys, yr, zns, znr, zos, zor, zfs, zfr,
          eys, eyr, ens, enr, eos, eor, efs, efr,
          obuf, kvsem, qsem, osem, ss, rq, rr):
    nc = CHUNKS
    bc = nb // nc
    pitch = bc + 8
    rows = 16 * own
    half = rows // 2
    scale = dim ** -0.5
    me = lax.axis_index("dup")
    core, yy, zz = me % 2, (me // 2) % 2, me // 4
    inner = ((zz + 1) // 2) % 2
    partner = me + 1 - 2 * core
    ypeer = me + 2 - 4 * yy
    z1 = me + 4 * (1 - 2 * (zz % 2))
    z2 = me + 4 * (2 - 4 * (zz // 2))
    z3 = me + 4 * (3 - 2 * zz)
    far_inner = me + 4 * (2 - zz // 2 - zz)

    def upto(n):
        return pl.ds(0, n)

    def among(c, ways, way):
        hits = [c == k for k in range(nc) if ways[k] == way]
        return functools.reduce(jnp.logical_or, hits, jnp.bool_(False))

    def by_way(ways, fns):
        def run(c):
            for way, fn in fns.items():
                if fn is not None and way in ways:
                    pl.when(among(c, ways, way))(functools.partial(fn, c))
        return run

    def remote(src, dst, ssem, rsem, dev):
        return pltpu.make_async_remote_copy(src_ref=src, dst_ref=dst, send_sem=ssem, recv_sem=rsem,
                                            device_id={"dup": dev}, device_id_type=MESH)

    def send(src, dst, si, rsem, dev):
        remote(src, dst, ss.at[si], rsem, dev).start()

    def recv(ref, rsem):
        remote(ref, ref, ss.at[0], rsem, partner).wait_recv()

    def kv_copies(c):
        sl = pl.ds(c * bc, bc)
        return (pltpu.make_async_copy(k_ref.at[sl], kbuf.at[sl], kvsem.at[c]),
                pltpu.make_async_copy(v_ref.at[sl], vbuf.at[sl], kvsem.at[c]))

    def own_q(c):
        return pltpu.make_async_copy(q_ref.at[:, pl.ds(c * bc, bc)], qbuf.at[c, 0, 0, 0], qsem)

    def start_q(c, carry):
        own_q(c).start()
        return carry

    def start_kv(c, carry):
        for cp in kv_copies(c):
            cp.start()
        return carry

    lax.fori_loop(0, nc, start_q, 0)
    lax.fori_loop(0, nc, start_kv, 0)

    barrier = pltpu.get_barrier_semaphore()
    peers = (partner, ypeer, z1, z2, z3)
    for dev in peers:
        pl.semaphore_signal(barrier, inc=1, device_id={"dup": dev}, device_id_type=MESH)

    rowid = lax.broadcasted_iota(jnp.int32, (rows, span), 0)
    lane = lax.broadcasted_iota(jnp.int32, (rows, span), 1)
    slot = (rowid * 171) >> 9
    item = rowid - 3 * slot
    rel = (slot & 3) * 4 + ((slot >> 2) & 1) * 2 + (slot >> 3)
    tok = (own * (rel ^ me) + item) & 3
    posm[...] = me * span + lane + 4 - tok
    ltmp[...] = jnp.zeros_like(ltmp)

    pltpu.make_async_copy(q_ref, q_ref, qsem).wait()
    pl.semaphore_wait(barrier, len(peers))

    def q_far(c, ny):
        y = upto(ny)
        send(qbuf.at[c, 0, y, 0], qbuf.at[c, 0, y, 2 + inner], ny + ny - 1, rq.at[1, c], far_inner)
        pl.when(inner == 0)(lambda: q_near(c, ny))

    def q_near(c, ny):
        y = upto(ny)
        send(qbuf.at[c, 0, y, 0], qbuf.at[c, 0, y, 1], ny + ny - 1, rq.at[0, c], z1)

    def q_relayed(c, ny):
        recv(qbuf.at[c, 0, upto(ny), pl.ds(2, 2)], rq.at[1, c])

    def q_relay(c, ny):
        @pl.when(inner == 1)
        def _():
            y = upto(ny)
            q_relayed(c, ny)
            send(qbuf.at[c, 0, y, 2], qbuf.at[c, 0, y, 3], 2 * ny, rq.at[1, c], z1)
            send(qbuf.at[c, 0, y, 3], qbuf.at[c, 0, y, 2], 2 * ny, rq.at[1, c], z1)
            q_near(c, ny)

    def q_end(c, ny):
        pl.when(inner == 0)(lambda: q_relayed(c, ny))
        recv(qbuf.at[c, 0, upto(ny), 1], rq.at[0, c])

    def q_y_own(c, si=5):
        send(qbuf.at[c, 0, 0, 0], qbuf.at[c, 0, 1, 0], si, rq.at[2, c], ypeer)

    def q_y_rest(c):
        z = pl.ds(1, 3)
        send(qbuf.at[c, 0, 0, z], qbuf.at[c, 0, 1, z], 5, rq.at[2, c], ypeer)

    def q_partner(c):
        send(qbuf.at[c, 0], qbuf.at[c, 1], 7, rq.at[3, c], partner)

    def q_last(c):
        recv(qbuf.at[c, 0, 1], rq.at[2, c])
        q_partner(c)

    def both(*fns):
        def run(c):
            for fn in fns:
                fn(c)
        return run

    y_own = by_way(Q_WAY, {"A": q_y_own, "B": lambda c: q_y_own(c, 6)})
    q0 = by_way(Q_WAY, {"A": lambda c: q_far(c, 1)})
    q1 = by_way(Q_WAY, {
        "A": lambda c: q_relay(c, 1),
        "B": both(lambda c: recv(qbuf.at[c, 0, 1, 0], rq.at[2, c]), lambda c: q_far(c, 2))})
    q2 = by_way(Q_WAY, {
        "A": both(lambda c: q_end(c, 1), q_y_rest),
        "B": lambda c: q_relay(c, 2)})
    q3 = by_way(Q_WAY, {
        "A": q_last,
        "B": both(lambda c: q_end(c, 2), q_partner)})

    def compute(c):
        recv(qbuf.at[c, 1], rq.at[3, c])
        for s in range(16):
            for i in range(own):
                qf[pl.ds((s * own + i) * pitch, bc), :] = qbuf[c, s // 8, (s // 4) % 2, s % 4, i].astype(F32)
        pltpu.make_async_copy(k_ref.at[pl.ds(0, 2 * bc)], kbuf.at[pl.ds(0, 2 * bc)], kvsem.at[c]).wait()
        base = (c % 2) * (rows * pitch)
        macc[...] = jnp.zeros_like(macc)
        dacc[...] = jnp.zeros_like(dacc)
        place = lax.broadcasted_iota(jnp.int32, (rows, 128), 1)
        rid = lax.broadcasted_iota(jnp.int32, (rows, 128), 0)
        place = place - bc * (rid - 3 * ((rid * 171) >> 9))

        def scores(j):
            qb = qf[pl.ds(j, rows, stride=pitch), :].astype(BF16)
            sbuf[j] = lax.dot_general(qb, kbuf[c * bc + j], (((1,), (1,)), ((), ())), preferred_element_type=F32)

        def soften(j, mv, dv):
            s = jnp.where(posm[...] <= len_ref[c * bc + j], sbuf[j], NEG)
            mx = jnp.maximum(jnp.max(s, axis=1, keepdims=True), FLOOR)
            p = jnp.exp2((s - mx) * (scale * math.log2(math.e)))
            pbuf[j] = p.astype(BF16)
            hit = place == j
            return jnp.where(hit, mx, mv), jnp.where(hit, jnp.sum(p, axis=1, keepdims=True), dv)

        def soften_group(g, carry):
            mv, dv = macc[...], dacc[...]
            for u in range(UNROLL):
                mv, dv = soften(g * UNROLL + u, mv, dv)
            macc[...] = mv
            dacc[...] = dv
            return carry

        for j in range(bc):
            scores(j)
        lax.fori_loop(0, bc // UNROLL, soften_group, 0)
        for j in range(bc):
            of[pl.ds(base + j, rows, stride=pitch), :] = jnp.dot(pbuf[j], vbuf[c * bc + j], preferred_element_type=F32)
        for t, acc in ((0, macc), (1, dacc)):
            line = acc[pl.ds(0, 16, stride=3), :] + acc[pl.ds(1, 16, stride=3), :] + acc[pl.ds(2, 16, stride=3), :]
            if t == 0:
                line = line * scale
            e1k[c, t] = line[:8]
            e1s[c, t] = line[8:]
        for r in range(half):
            p1s[c, r] = of[pl.ds(base + (half + r) * pitch, bc), :].astype(BF16)
        send(e1s.at[c], e1r.at[c], 9, rr.at[1, c], partner)
        send(p1s.at[c], p1r.at[c], 8, rr.at[0, c], partner)

    def finish(c, i, o):
        obuf[c, i] = o.astype(BF16)

    def ship(c):
        pltpu.make_async_copy(obuf.at[c], out_ref.at[:, pl.ds(c * bc, bc)], osem).start()

    def cut(w, line, i):
        return w[i * bc:(i + 1) * bc, line:line + 1]

    def lines(refs):
        for n, ref in refs:
            ltmp[n:n + 1] = ref
        return ltmp[...]

    def weights(*ls):
        top = functools.reduce(jnp.maximum, ls)
        es = [jnp.exp(x - top) for x in ls]
        tot = functools.reduce(lambda a, b: a + b, es)
        inv = 1.0 / tot
        return [(e * inv).T for e in es], top + jnp.log(tot)

    def merge_partner(c):
        recv(e1r.at[c], rr.at[1, c])
        ma, mb = e1k[c, 0], e1r[c, 0]
        top = jnp.maximum(ma, mb)
        ea, eb = jnp.exp(ma - top), jnp.exp(mb - top)
        tot = jnp.maximum(ea * e1k[c, 1] + eb * e1r[c, 1], 1.0)
        inv = 1.0 / tot
        lse[c] = top + jnp.log(tot)
        wa, wb = (ea * inv).T, (eb * inv).T
        recv(p1r.at[c], rr.at[0, c])
        base = (c % 2) * (rows * pitch)
        for n in range(8):
            for i in range(own):
                r = n * own + i
                part[c, n, i] = (cut(wa, n, i) * of[pl.ds(base + r * pitch, bc), :]
                                 + cut(wb, n, i) * p1r[c, r].astype(F32))

    def y_send(c, ny):
        for z in range(4 if ny == 1 else 1):
            eys[c, z] = lse[c, 4 + z:5 + z]
            for i in range(own):
                ys[c, z, i] = part[c, 4 + z, i].astype(BF16)
        if ny == 1:
            send(eys.at[c], eyr.at[c], 11, rr.at[3, c], ypeer)
            send(ys.at[c], yr.at[c], 10, rr.at[2, c], ypeer)
        else:
            send(eys.at[c, 0], eyr.at[c, 0], 13, rr.at[3, c], ypeer)
            send(ys.at[c, 0], yr.at[c, 0], 12, rr.at[2, c], ypeer)

    def y_merge(c, ny):
        if ny == 1:
            recv(eyr.at[c], rr.at[3, c])
            (wa, wb), new = weights(lse[c], lines([(z, eyr[c, z]) for z in range(4)]))
            lse[c] = new
            recv(yr.at[c], rr.at[2, c])
            for z in range(4):
                for i in range(own):
                    part[c, z, i] = cut(wa, z, i) * part[c, z, i] + cut(wb, z, i) * yr[c, z, i].astype(F32)
        else:
            recv(eyr.at[c, 0], rr.at[3, c])
            (wa, wb), _ = weights(lse[c], lines([(0, eyr[c, 0])]))
            recv(yr.at[c, 0], rr.at[2, c])
            for i in range(own):
                finish(c, i, cut(wa, 0, i) * part[c, 0, i] + cut(wb, 0, i) * yr[c, 0, i].astype(F32))
            ship(c)

    def z_send(c, ny):
        y = upto(ny)

        @pl.when(inner == 0)
        def _():
            for m in range(2):
                for h in range(ny):
                    eos[c, m, h] = lse[c, 4 * h + 2 + m:4 * h + 3 + m]
                    for i in range(own):
                        zos[c, m, h, i] = part[c, 4 * h + 2 + m, i].astype(BF16)
            send(eos.at[c, :, y], eor.at[c, :, y], 17 + ny + ny, rr.at[7, c], z1)
            send(zos.at[c, :, y], zor.at[c, :, y], 16 + ny + ny, rr.at[6, c], z1)

        for h in range(ny):
            ens[c, h] = lse[c, 4 * h + 1:4 * h + 2]
            for i in range(own):
                zns[c, h, i] = part[c, 4 * h + 1, i].astype(BF16)
        send(ens.at[c, y], enr.at[c, y], 13 + ny + ny, rr.at[5, c], z1)
        send(zns.at[c, y], znr.at[c, y], 12 + ny + ny, rr.at[4, c], z1)

    def z_send_direct(c):
        for k, dat, lin in ((2, zos.at[c, 0, 0], eos.at[c, 0, 0]), (3, zos.at[c, 1, 0], eos.at[c, 1, 0]),
                            (1, zns.at[c, 0], ens.at[c, 0])):
            lin[...] = lse[c, k:k + 1]
            for i in range(own):
                dat[i] = part[c, k, i].astype(BF16)
        for m, dev in ((1, z3), (0, z2)):
            send(eos.at[c, m, 0], eor.at[c, m, 0], 19, rr.at[7, c], dev)
            send(zos.at[c, m, 0], zor.at[c, m, 0], 18, rr.at[6, c], dev)
        send(ens.at[c, 0], enr.at[c, 0], 15, rr.at[5, c], z1)
        send(zns.at[c, 0], znr.at[c, 0], 14, rr.at[4, c], z1)

    def z_merge_direct(c):
        recv(enr.at[c, 0], rr.at[5, c])
        recv(eor.at[c, :, 0], rr.at[7, c])
        ls = [lines([(0, ref)]) for ref in (enr[c, 0], eor[c, 0, 0], eor[c, 1, 0])]
        ws, _ = weights(lse[c], *ls)
        recv(znr.at[c, 0], rr.at[4, c])
        recv(zor.at[c, :, 0], rr.at[6, c])
        for i in range(own):
            o = cut(ws[0], 0, i) * part[c, 0, i]
            for w, dat in zip(ws[1:], (znr.at[c, 0], zor.at[c, 0, 0], zor.at[c, 1, 0])):
                o = o + cut(w, 0, i) * dat[i].astype(F32)
            finish(c, i, o)
        ship(c)

    def z_relay(c, ny):
        y = upto(ny)
        recv(eor.at[c, :, y], rr.at[7, c])
        (wa, wb), new = weights(lse[c], lines([(4 * h + 3 - m, eor[c, m, h]) for m in range(2) for h in range(ny)]))
        recv(zor.at[c, :, y], rr.at[6, c])
        for m in range(2):
            for h in range(ny):
                n = 4 * h + 3 - m
                efs[c, m, h] = new[n:n + 1]
                for i in range(own):
                    o = cut(wa, n, i) * part[c, n, i] + cut(wb, n, i) * zor[c, m, h, i].astype(F32)
                    zfs[c, m, h, i] = o.astype(BF16)
        for m, dev in ((1, z2), (0, z3)):
            send(efs.at[c, m, y], efr.at[c, y], 21 + ny + ny, rr.at[9, c], dev)
            send(zfs.at[c, m, y], zfr.at[c, y], 20 + ny + ny, rr.at[8, c], dev)

    def z_merge(c, ny):
        y = upto(ny)
        recv(enr.at[c, y], rr.at[5, c])
        recv(efr.at[c, y], rr.at[9, c])
        near = lines([(4 * h, enr[c, h]) for h in range(ny)])
        far = lines([(4 * h, efr[c, h]) for h in range(ny)])
        (wa, wb, wc), new = weights(lse[c], near, far)
        lse[c] = new
        recv(znr.at[c, y], rr.at[4, c])
        recv(zfr.at[c, y], rr.at[8, c])
        for h in range(ny):
            n = 4 * h
            for i in range(own):
                o = (cut(wa, n, i) * part[c, n, i] + cut(wb, n, i) * znr[c, h, i].astype(F32)
                     + cut(wc, n, i) * zfr[c, h, i].astype(F32))
                if ny == 1:
                    finish(c, i, o)
                else:
                    part[c, n, i] = o
        if ny == 1:
            ship(c)

    r0_send = by_way(O_WAY, {"D": lambda c: y_send(c, 1), "A": lambda c: y_send(c, 1), "B": lambda c: z_send(c, 2)})

    def r0(c):
        merge_partner(c)
        r0_send(c)

    def relay(c, ny):
        pl.when(inner == 1)(lambda: z_relay(c, ny))

    r1 = by_way(O_WAY, {
        "D": both(lambda c: y_merge(c, 1), z_send_direct),
        "A": both(lambda c: y_merge(c, 1), lambda c: z_send(c, 1)),
        "B": lambda c: relay(c, 2)})
    r2 = by_way(O_WAY, {
        "D": None,
        "A": lambda c: relay(c, 1),
        "B": both(lambda c: z_merge(c, 2), lambda c: y_send(c, 2))})
    r3 = by_way(O_WAY, {
        "D": z_merge_direct,
        "A": lambda c: z_merge(c, 1),
        "B": lambda c: y_merge(c, 2)})

    def at(c, fn):
        pl.when((c >= 0) & (c < nc))(lambda: fn(c))

    def first(c, carry):
        pl.when(c < AHEAD)(lambda: q0(c))
        y_own(c)
        return carry

    lax.fori_loop(0, Y_AHEAD, first, 0)

    def step(st, carry):
        at(st + AHEAD, q0)
        at(st + Y_AHEAD, y_own)
        at(st - LAG[0], q1)
        at(st - LAG[1], q2)
        at(st - LAG[2], q3)
        at(st - LAG[3], compute)
        at(st - LAG[4], r0)
        at(st - LAG[5], r1)
        at(st - LAG[6], r2)
        at(st - LAG[7], r3)
        return carry

    lax.fori_loop(0, nc + LAG[7], step, 0)

    def sent(ref, si):
        remote(ref, ref, ss.at[si], rq.at[0, 0], partner).wait_send()

    def sent_of(n, *pairs):
        if n:
            for fn, si in pairs:
                sent(fn(upto(n)), si)

    na, nbb = (Q_WAY.count(w) for w in "AB")
    sent_of(na, (lambda c: qbuf.at[c, 0, 0, upto(2)], 1))
    sent_of(nbb, (lambda c: qbuf.at[c, 0, :, upto(2)], 3), (lambda c: qbuf.at[c, 0, 0, 0], 6))
    sent_of(na, (lambda c: qbuf.at[c, 0, 0], 5))

    @pl.when(inner == 1)
    def _():
        sent_of(na, (lambda c: qbuf.at[c, 0, 0, upto(2)], 2))
        sent_of(nbb, (lambda c: qbuf.at[c, 0, :, upto(2)], 4))

    sent(qbuf.at[:, 0], 7)
    od, oa, ob = (O_WAY.count(w) for w in "DAB")
    sent_of(od + oa, (lambda c: ys.at[c], 10), (lambda c: eys.at[c], 11),
            (lambda c: zns.at[c, 0], 14), (lambda c: ens.at[c, 0], 15))
    sent_of(ob, (lambda c: ys.at[c, 0], 12), (lambda c: eys.at[c, 0], 13),
            (lambda c: zns.at[c], 16), (lambda c: ens.at[c], 17))

    @pl.when(inner == 0)
    def _():
        sent_of(od + oa, (lambda c: zos.at[c, :, 0], 18), (lambda c: eos.at[c, :, 0], 19))
        sent_of(ob, (lambda c: zos.at[c], 20), (lambda c: eos.at[c], 21))

    @pl.when(inner == 1)
    def _():
        sent_of(od, (lambda c: zos.at[c, :, 0], 18), (lambda c: eos.at[c, :, 0], 19))
        sent_of(oa, (lambda c: zfs.at[c, :, 0], 22), (lambda c: efs.at[c, :, 0], 23))
        sent_of(ob, (lambda c: zfs.at[c], 24), (lambda c: efs.at[c], 25))

    sent(p1s, 8)
    sent(e1s, 9)
    pltpu.make_async_copy(out_ref, out_ref, osem).wait()


def solution(mesh):
    def group_step(q_local, k_span, v_span, len_local):
        nb, own, dim = q_local.shape
        span = k_span.shape[1]
        rows = 16 * own
        half = rows // 2
        nc = CHUNKS
        bc = nb // nc
        pitch = bc + 8
        q_planes = jnp.transpose(q_local, (1, 0, 2))
        vm = pltpu.VMEM
        dma = pltpu.SemaphoreType.DMA
        any_spec = pl.BlockSpec(memory_space=pl.ANY)

        def blocks(*lead):
            return vm((nc, *lead, own, bc, dim), BF16)

        def line(*lead):
            return vm((nc, *lead, 1, 128), F32)

        out = pl.pallas_call(
            functools.partial(fused, nb, own, span, dim),
            out_shape=jax.ShapeDtypeStruct((own, nb, dim), BF16),
            in_specs=[pl.BlockSpec(memory_space=pltpu.SMEM), any_spec, any_spec, any_spec],
            out_specs=any_spec,
            scratch_shapes=[
                vm((nb, span, dim), BF16), vm((nb, span, dim), BF16),
                blocks(2, 2, 4),
                vm((rows * pitch, dim), F32), vm((2 * rows * pitch, dim), F32),
                vm((rows, span), jnp.int32), vm((rows, 128), F32), vm((rows, 128), F32),
                vm((bc, rows, span), F32), vm((bc, rows, span), BF16),
                vm((nc, half, bc, dim), BF16), vm((nc, half, bc, dim), BF16),
                vm((nc, 2, 8, 128), F32), vm((nc, 2, 8, 128), F32), vm((nc, 2, 8, 128), F32),
                vm((nc, 8, own, bc, dim), F32), vm((nc, 8, 128), F32), vm((8, 128), F32),
                blocks(4), blocks(4), blocks(2), blocks(2),
                blocks(2, 2), blocks(2, 2), blocks(2, 2), blocks(2),
                line(4), line(4), line(2), line(2), line(2, 2), line(2, 2), line(2, 2), line(2),
                blocks(), dma((nc,)), dma, dma, dma((26,)), dma((4, nc)), dma((10, nc)),
            ],
            compiler_params=pltpu.CompilerParams(
                collective_id=0, has_side_effects=True, vmem_limit_bytes=67043328),
            name="attend",
        )(len_local, q_planes, k_span, v_span)
        return jnp.transpose(out, (1, 0, 2))

    return jax.shard_map(group_step, mesh=mesh, in_specs=(P("kv", "dup", None), P("kv", "dup", None), P("kv", "dup", None), P("kv")), out_specs=P("kv", "dup", None), check_vma=False)
```

```python
import functools
import math

import jax
import jax.numpy as jnp
from jax import lax
from jax.experimental import pallas as pl
from jax.experimental.pallas import tpu as pltpu
from jax.sharding import PartitionSpec as P

CHUNKS = 8
UNROLL = 32
AHEAD = 2
Y_AHEAD = 3
LAG = (0, 1, 3, 4, 5, 7, 11)
Q_WAY = "AAABAABA"
O_WAY = "DDDDDDDD"
NEG = -3.4e38
FLOOR = -3.0e38
MESH = pl.DeviceIdType.MESH
F32 = jnp.float32
BF16 = jnp.bfloat16
def fused(nb, own, span, dim, len_ref, q_ref, k_ref, v_ref, out_ref,
          kbuf, vbuf, qbuf, qf, of, posm, macc, dacc, sbuf, pbuf,
          p1s, p1r, e1k, e1s, e1r, part, lse, ltmp,
          ys, yr, zns, znr, zos, zor,
          eys, eyr, ens, enr, eos, eor,
          obuf, kvsem, qsem, osem, ss, rq, rr):
    nc = CHUNKS
    bc = nb // nc
    pitch = bc + 8
    rows = 16 * own
    half = rows // 2
    scale = dim ** -0.5
    me = lax.axis_index("dup")
    core, yy, zz = me % 2, (me // 2) % 2, me // 4
    inner = ((zz + 1) // 2) % 2
    partner = me + 1 - 2 * core
    ypeer = me + 2 - 4 * yy
    z1 = me + 4 * (1 - 2 * (zz % 2))
    z2 = me + 4 * (2 - 4 * (zz // 2))
    z3 = me + 4 * (3 - 2 * zz)
    far_inner = me + 4 * (2 - zz // 2 - zz)

    def upto(n):
        return pl.ds(0, n)

    def among(c, ways, way):
        hits = [c == k for k in range(nc) if ways[k] == way]
        return functools.reduce(jnp.logical_or, hits, jnp.bool_(False))

    def by_way(ways, fns):
        def run(c):
            for way, fn in fns.items():
                if fn is not None and way in ways:
                    pl.when(among(c, ways, way))(functools.partial(fn, c))
        return run

    def remote(src, dst, ssem, rsem, dev):
        return pltpu.make_async_remote_copy(src_ref=src, dst_ref=dst, send_sem=ssem, recv_sem=rsem,
                                            device_id={"dup": dev}, device_id_type=MESH)

    def send(src, dst, si, rsem, dev):
        remote(src, dst, ss.at[si], rsem, dev).start()

    def recv(ref, rsem):
        remote(ref, ref, ss.at[0], rsem, partner).wait_recv()

    def kv_copies(c):
        sl = pl.ds(c * bc, bc)
        return (pltpu.make_async_copy(k_ref.at[sl], kbuf.at[sl], kvsem.at[c]),
                pltpu.make_async_copy(v_ref.at[sl], vbuf.at[sl], kvsem.at[c]))

    def own_q(c):
        return pltpu.make_async_copy(q_ref.at[:, pl.ds(c * bc, bc)], qbuf.at[c, 0, 0, 0], qsem)

    def start_q(c, carry):
        own_q(c).start()
        return carry

    def start_kv(c, carry):
        for cp in kv_copies(c):
            cp.start()
        return carry

    lax.fori_loop(0, nc, start_q, 0)
    lax.fori_loop(0, nc, start_kv, 0)

    barrier = pltpu.get_barrier_semaphore()
    peers = (partner, ypeer, z1, z2, z3)
    for dev in peers:
        pl.semaphore_signal(barrier, inc=1, device_id={"dup": dev}, device_id_type=MESH)

    rowid = lax.broadcasted_iota(jnp.int32, (rows, span), 0)
    lane = lax.broadcasted_iota(jnp.int32, (rows, span), 1)
    slot = (rowid * 171) >> 9
    item = rowid - 3 * slot
    rel = (slot & 3) * 4 + ((slot >> 2) & 1) * 2 + (slot >> 3)
    tok = (own * (rel ^ me) + item) & 3
    posm[...] = me * span + lane + 4 - tok
    ltmp[...] = jnp.zeros_like(ltmp)

    pltpu.make_async_copy(q_ref, q_ref, qsem).wait()
    pl.semaphore_wait(barrier, len(peers))

    def q_far(c, ny):
        y = upto(ny)
        send(qbuf.at[c, 0, y, 0], qbuf.at[c, 0, y, 2 + inner], ny + ny - 1, rq.at[1, c], far_inner)
        pl.when(inner == 0)(lambda: q_near(c, ny))

    def q_near(c, ny):
        y = upto(ny)
        send(qbuf.at[c, 0, y, 0], qbuf.at[c, 0, y, 1], ny + ny - 1, rq.at[0, c], z1)

    def q_relayed(c, ny):
        recv(qbuf.at[c, 0, upto(ny), pl.ds(2, 2)], rq.at[1, c])

    def q_relay(c, ny):
        @pl.when(inner == 1)
        def _():
            y = upto(ny)
            q_relayed(c, ny)
            send(qbuf.at[c, 0, y, 2], qbuf.at[c, 0, y, 3], 2 * ny, rq.at[1, c], z1)
            send(qbuf.at[c, 0, y, 3], qbuf.at[c, 0, y, 2], 2 * ny, rq.at[1, c], z1)
            q_near(c, ny)

    def q_end(c, ny):
        pl.when(inner == 0)(lambda: q_relayed(c, ny))
        recv(qbuf.at[c, 0, upto(ny), 1], rq.at[0, c])

    def q_y_own(c, si=5):
        send(qbuf.at[c, 0, 0, 0], qbuf.at[c, 0, 1, 0], si, rq.at[2, c], ypeer)

    def q_y_rest(c):
        z = pl.ds(1, 3)
        send(qbuf.at[c, 0, 0, z], qbuf.at[c, 0, 1, z], 5, rq.at[2, c], ypeer)

    def q_partner(c):
        send(qbuf.at[c, 0], qbuf.at[c, 1], 7, rq.at[3, c], partner)

    def q_last(c):
        recv(qbuf.at[c, 0, 1], rq.at[2, c])
        q_partner(c)

    def both(*fns):
        def run(c):
            for fn in fns:
                fn(c)
        return run

    y_own = by_way(Q_WAY, {"A": q_y_own, "B": lambda c: q_y_own(c, 6)})
    q0 = by_way(Q_WAY, {"A": lambda c: q_far(c, 1)})
    q1 = by_way(Q_WAY, {
        "A": lambda c: q_relay(c, 1),
        "B": both(lambda c: recv(qbuf.at[c, 0, 1, 0], rq.at[2, c]), lambda c: q_far(c, 2))})
    q2 = by_way(Q_WAY, {
        "A": both(lambda c: q_end(c, 1), q_y_rest),
        "B": lambda c: q_relay(c, 2)})
    q3 = by_way(Q_WAY, {
        "A": q_last,
        "B": both(lambda c: q_end(c, 2), q_partner)})

    def compute(c):
        recv(qbuf.at[c, 1], rq.at[3, c])
        for s in range(16):
            for i in range(own):
                qf[pl.ds((s * own + i) * pitch, bc), :] = qbuf[c, s // 8, (s // 4) % 2, s % 4, i].astype(F32)
        pltpu.make_async_copy(k_ref.at[pl.ds(0, 2 * bc)], kbuf.at[pl.ds(0, 2 * bc)], kvsem.at[c]).wait()
        base = (c % 2) * (rows * pitch)
        macc[...] = jnp.zeros_like(macc)
        dacc[...] = jnp.zeros_like(dacc)
        place = lax.broadcasted_iota(jnp.int32, (rows, 128), 1)
        rid = lax.broadcasted_iota(jnp.int32, (rows, 128), 0)
        place = place - bc * (rid - 3 * ((rid * 171) >> 9))

        def scores(j):
            qb = qf[pl.ds(j, rows, stride=pitch), :].astype(BF16)
            sbuf[j] = lax.dot_general(qb, kbuf[c * bc + j], (((1,), (1,)), ((), ())), preferred_element_type=F32)

        def soften(j, mv, dv):
            s = jnp.where(posm[...] <= len_ref[c * bc + j], sbuf[j], NEG)
            mx = jnp.maximum(jnp.max(s, axis=1, keepdims=True), FLOOR)
            p = jnp.exp2((s - mx) * (scale * math.log2(math.e)))
            pbuf[j] = p.astype(BF16)
            hit = place == j
            return jnp.where(hit, mx, mv), jnp.where(hit, jnp.sum(p, axis=1, keepdims=True), dv)

        def soften_group(g, carry):
            mv, dv = macc[...], dacc[...]
            for u in range(UNROLL):
                mv, dv = soften(g * UNROLL + u, mv, dv)
            macc[...] = mv
            dacc[...] = dv
            return carry

        for j in range(bc):
            scores(j)
        lax.fori_loop(0, bc // UNROLL, soften_group, 0)
        for j in range(bc):
            of[pl.ds(base + j, rows, stride=pitch), :] = jnp.dot(pbuf[j], vbuf[c * bc + j], preferred_element_type=F32)
        for t, acc in ((0, macc), (1, dacc)):
            line = acc[pl.ds(0, 16, stride=3), :] + acc[pl.ds(1, 16, stride=3), :] + acc[pl.ds(2, 16, stride=3), :]
            if t == 0:
                line = line * scale
            e1k[c, t] = line[:8]
            e1s[c, t] = line[8:]
        for r in range(half):
            p1s[c, r] = of[pl.ds(base + (half + r) * pitch, bc), :].astype(BF16)
        send(e1s.at[c], e1r.at[c], 9, rr.at[1, c], partner)
        send(p1s.at[c], p1r.at[c], 8, rr.at[0, c], partner)

    def finish(c, i, o):
        obuf[c, i] = o.astype(BF16)

    def ship(c):
        pltpu.make_async_copy(obuf.at[c], out_ref.at[:, pl.ds(c * bc, bc)], osem).start()

    def cut(w, line, i):
        return w[i * bc:(i + 1) * bc, line:line + 1]

    def lines(refs):
        for n, ref in refs:
            ltmp[n:n + 1] = ref
        return ltmp[...]

    def weights(*ls):
        top = functools.reduce(jnp.maximum, ls)
        es = [jnp.exp(x - top) for x in ls]
        tot = functools.reduce(lambda a, b: a + b, es)
        inv = 1.0 / tot
        return [(e * inv).T for e in es], top + jnp.log(tot)

    def merge_partner(c):
        recv(e1r.at[c], rr.at[1, c])
        ma, mb = e1k[c, 0], e1r[c, 0]
        top = jnp.maximum(ma, mb)
        ea, eb = jnp.exp(ma - top), jnp.exp(mb - top)
        tot = jnp.maximum(ea * e1k[c, 1] + eb * e1r[c, 1], 1.0)
        inv = 1.0 / tot
        lse[c] = top + jnp.log(tot)
        wa, wb = (ea * inv).T, (eb * inv).T
        recv(p1r.at[c], rr.at[0, c])
        base = (c % 2) * (rows * pitch)
        for n in range(8):
            for i in range(own):
                r = n * own + i
                part[c, n, i] = (cut(wa, n, i) * of[pl.ds(base + r * pitch, bc), :]
                                 + cut(wb, n, i) * p1r[c, r].astype(F32))

    def y_send(c, ny):
        for z in range(4 if ny == 1 else 1):
            eys[c, z] = lse[c, 4 + z:5 + z]
            for i in range(own):
                ys[c, z, i] = part[c, 4 + z, i].astype(BF16)
        if ny == 1:
            send(eys.at[c], eyr.at[c], 11, rr.at[3, c], ypeer)
            send(ys.at[c], yr.at[c], 10, rr.at[2, c], ypeer)
        else:
            send(eys.at[c, 0], eyr.at[c, 0], 13, rr.at[3, c], ypeer)
            send(ys.at[c, 0], yr.at[c, 0], 12, rr.at[2, c], ypeer)

    def y_merge(c, ny):
        if ny == 1:
            recv(eyr.at[c], rr.at[3, c])
            (wa, wb), new = weights(lse[c], lines([(z, eyr[c, z]) for z in range(4)]))
            lse[c] = new
            recv(yr.at[c], rr.at[2, c])
            for z in range(4):
                for i in range(own):
                    part[c, z, i] = cut(wa, z, i) * part[c, z, i] + cut(wb, z, i) * yr[c, z, i].astype(F32)
        else:
            recv(eyr.at[c, 0], rr.at[3, c])
            (wa, wb), _ = weights(lse[c], lines([(0, eyr[c, 0])]))
            recv(yr.at[c, 0], rr.at[2, c])
            for i in range(own):
                finish(c, i, cut(wa, 0, i) * part[c, 0, i] + cut(wb, 0, i) * yr[c, 0, i].astype(F32))
            ship(c)

    def z_send(c, ny):
        y = upto(ny)
        for k, dat, lin in ((3, zos.at[c, 1], eos.at[c, 1]), (2, zos.at[c, 0], eos.at[c, 0]), (1, zns.at[c], ens.at[c])):
            for h in range(ny):
                lin[h] = lse[c, 4 * h + k:4 * h + k + 1]
                for i in range(own):
                    dat[h, i] = part[c, 4 * h + k, i].astype(BF16)
        for m, dev in ((1, z3), (0, z2)):
            send(eos.at[c, m, y], eor.at[c, m, y], 17 + ny + ny, rr.at[7, c], dev)
            send(zos.at[c, m, y], zor.at[c, m, y], 16 + ny + ny, rr.at[6, c], dev)
        send(ens.at[c, y], enr.at[c, y], 13 + ny + ny, rr.at[5, c], z1)
        send(zns.at[c, y], znr.at[c, y], 12 + ny + ny, rr.at[4, c], z1)

    def z_merge(c, ny):
        y = upto(ny)
        recv(enr.at[c, y], rr.at[5, c])
        recv(eor.at[c, :, y], rr.at[7, c])
        came = ((znr.at[c], enr.at[c]), (zor.at[c, 0], eor.at[c, 0]), (zor.at[c, 1], eor.at[c, 1]))
        ws, new = weights(lse[c], *[lines([(4 * h, lin[h]) for h in range(ny)]) for _, lin in came])
        recv(znr.at[c, y], rr.at[4, c])
        recv(zor.at[c, :, y], rr.at[6, c])
        for h in range(ny):
            for i in range(own):
                o = cut(ws[0], 4 * h, i) * part[c, 4 * h, i]
                for w, (dat, _) in zip(ws[1:], came):
                    o = o + cut(w, 4 * h, i) * dat[h, i].astype(F32)
                if ny == 1:
                    finish(c, i, o)
                else:
                    part[c, 4 * h, i] = o
        if ny == 1:
            ship(c)
        else:
            lse[c] = new

    r0_send = by_way(O_WAY, {"D": lambda c: y_send(c, 1), "E": lambda c: z_send(c, 2)})

    def r0(c):
        merge_partner(c)
        r0_send(c)

    r1 = by_way(O_WAY, {
        "D": both(lambda c: y_merge(c, 1), lambda c: z_send(c, 1)),
        "E": both(lambda c: z_merge(c, 2), lambda c: y_send(c, 2))})
    r2 = by_way(O_WAY, {"D": lambda c: z_merge(c, 1), "E": lambda c: y_merge(c, 2)})

    def at(c, fn):
        pl.when((c >= 0) & (c < nc))(lambda: fn(c))

    def first(c, carry):
        pl.when(c < AHEAD)(lambda: q0(c))
        y_own(c)
        return carry

    lax.fori_loop(0, Y_AHEAD, first, 0)

    def step(st, carry):
        at(st + AHEAD, q0)
        at(st + Y_AHEAD, y_own)
        at(st - LAG[0], q1)
        at(st - LAG[1], q2)
        at(st - LAG[2], q3)
        at(st - LAG[3], compute)
        at(st - LAG[4], r0)
        at(st - LAG[5], r1)
        at(st - LAG[6], r2)
        return carry

    lax.fori_loop(0, nc + LAG[6], step, 0)

    def sent(ref, si):
        remote(ref, ref, ss.at[si], rq.at[0, 0], partner).wait_send()

    def sent_of(n, *pairs):
        if n:
            for fn, si in pairs:
                sent(fn(upto(n)), si)

    na, nbb = (Q_WAY.count(w) for w in "AB")
    sent_of(na, (lambda c: qbuf.at[c, 0, 0, upto(2)], 1))
    sent_of(nbb, (lambda c: qbuf.at[c, 0, :, upto(2)], 3), (lambda c: qbuf.at[c, 0, 0, 0], 6))
    sent_of(na, (lambda c: qbuf.at[c, 0, 0], 5))

    @pl.when(inner == 1)
    def _():
        sent_of(na, (lambda c: qbuf.at[c, 0, 0, upto(2)], 2))
        sent_of(nbb, (lambda c: qbuf.at[c, 0, :, upto(2)], 4))

    sent(qbuf.at[:, 0], 7)
    od, oe = (O_WAY.count(w) for w in "DE")
    sent_of(od, (lambda c: ys.at[c], 10), (lambda c: eys.at[c], 11),
            (lambda c: zns.at[c, 0], 14), (lambda c: ens.at[c, 0], 15),
            (lambda c: zos.at[c, :, 0], 18), (lambda c: eos.at[c, :, 0], 19))
    sent_of(oe, (lambda c: ys.at[c, 0], 12), (lambda c: eys.at[c, 0], 13),
            (lambda c: zns.at[c], 16), (lambda c: ens.at[c], 17),
            (lambda c: zos.at[c], 20), (lambda c: eos.at[c], 21))

    sent(p1s, 8)
    sent(e1s, 9)
    pltpu.make_async_copy(out_ref, out_ref, osem).wait()


def solution(mesh):
    def group_step(q_local, k_span, v_span, len_local):
        nb, own, dim = q_local.shape
        span = k_span.shape[1]
        rows = 16 * own
        half = rows // 2
        nc = CHUNKS
        bc = nb // nc
        pitch = bc + 8
        q_planes = jnp.transpose(q_local, (1, 0, 2))
        vm = pltpu.VMEM
        dma = pltpu.SemaphoreType.DMA
        any_spec = pl.BlockSpec(memory_space=pl.ANY)

        def blocks(*lead):
            return vm((nc, *lead, own, bc, dim), BF16)

        def line(*lead):
            return vm((nc, *lead, 1, 128), F32)

        out = pl.pallas_call(
            functools.partial(fused, nb, own, span, dim),
            out_shape=jax.ShapeDtypeStruct((own, nb, dim), BF16),
            in_specs=[pl.BlockSpec(memory_space=pltpu.SMEM), any_spec, any_spec, any_spec],
            out_specs=any_spec,
            scratch_shapes=[
                vm((nb, span, dim), BF16), vm((nb, span, dim), BF16),
                blocks(2, 2, 4),
                vm((rows * pitch, dim), F32), vm((2 * rows * pitch, dim), F32),
                vm((rows, span), jnp.int32), vm((rows, 128), F32), vm((rows, 128), F32),
                vm((bc, rows, span), F32), vm((bc, rows, span), BF16),
                vm((nc, half, bc, dim), BF16), vm((nc, half, bc, dim), BF16),
                vm((nc, 2, 8, 128), F32), vm((nc, 2, 8, 128), F32), vm((nc, 2, 8, 128), F32),
                vm((nc, 8, own, bc, dim), F32), vm((nc, 8, 128), F32), vm((8, 128), F32),
                blocks(4), blocks(4), blocks(2), blocks(2),
                blocks(2, 2), blocks(2, 2),
                line(4), line(4), line(2), line(2), line(2, 2), line(2, 2),
                blocks(), dma((nc,)), dma, dma, dma((22,)), dma((4, nc)), dma((8, nc)),
            ],
            compiler_params=pltpu.CompilerParams(
                collective_id=0, has_side_effects=True, vmem_limit_bytes=67043328),
            name="attend",
        )(len_local, q_planes, k_span, v_span)
        return jnp.transpose(out, (1, 0, 2))

    return jax.shard_map(group_step, mesh=mesh, in_specs=(P("kv", "dup", None), P("kv", "dup", None), P("kv", "dup", None), P("kv")), out_specs=P("kv", "dup", None), check_vma=False)
```

```python
import functools
import math

import jax
import jax.numpy as jnp
from jax import lax
from jax.experimental import pallas as pl
from jax.experimental.pallas import tpu as pltpu
from jax.sharding import PartitionSpec as P

CHUNKS = 8
UNROLL = 32
AHEAD = 2
Y_AHEAD = 3
LAG = (0, 1, 3, 4, 5, 7, 11)
Q_WAY = "AAABAABA"
O_WAY = "DDDDDDDD"
NEG = -3.4e38
FLOOR = -3.0e38
MESH = pl.DeviceIdType.MESH
F32 = jnp.float32
BF16 = jnp.bfloat16
def fused(nb, own, span, dim, len_ref, q_ref, k_ref, v_ref, out_ref,
          kbuf, vbuf, qbuf, qf, of, posm, macc, dacc, sbuf, pbuf,
          p1s, p1r, e1k, e1s, e1r, part, lse, ltmp,
          ys, yr, zns, znr, zos, zor,
          eys, eyr, ens, enr, eos, eor,
          obuf, kvsem, qsem, osem, ss, rq, rr):
    nc = CHUNKS
    bc = nb // nc
    pitch = bc + 8
    rows = 16 * own
    half = rows // 2
    scale = dim ** -0.5
    me = lax.axis_index("dup")
    core, yy, zz = me % 2, (me // 2) % 2, me // 4
    inner = ((zz + 1) // 2) % 2
    partner = me + 1 - 2 * core
    ypeer = me + 2 - 4 * yy
    z1 = me + 4 * (1 - 2 * (zz % 2))
    z2 = me + 4 * (2 - 4 * (zz // 2))
    z3 = me + 4 * (3 - 2 * zz)
    far_inner = me + 4 * (2 - zz // 2 - zz)

    def upto(n):
        return pl.ds(0, n)

    def among(c, ways, way):
        hits = [c == k for k in range(nc) if ways[k] == way]
        return functools.reduce(jnp.logical_or, hits, jnp.bool_(False))

    def by_way(ways, fns):
        def run(c):
            for way, fn in fns.items():
                if fn is not None and way in ways:
                    pl.when(among(c, ways, way))(functools.partial(fn, c))
        return run

    def remote(src, dst, ssem, rsem, dev):
        return pltpu.make_async_remote_copy(src_ref=src, dst_ref=dst, send_sem=ssem, recv_sem=rsem,
                                            device_id={"dup": dev}, device_id_type=MESH)

    def send(src, dst, si, rsem, dev):
        remote(src, dst, ss.at[si], rsem, dev).start()

    def recv(ref, rsem):
        remote(ref, ref, ss.at[0], rsem, partner).wait_recv()

    def kv_copies(c):
        sl = pl.ds(c * bc, bc)
        return (pltpu.make_async_copy(k_ref.at[sl], kbuf.at[sl], kvsem.at[c]),
                pltpu.make_async_copy(v_ref.at[sl], vbuf.at[sl], kvsem.at[c]))

    def own_q(c):
        return pltpu.make_async_copy(q_ref.at[:, pl.ds(c * bc, bc)], qbuf.at[c, 0, 0, 0], qsem)

    def start_q(c, carry):
        own_q(c).start()
        return carry

    def start_kv(c, carry):
        for cp in kv_copies(c):
            cp.start()
        return carry

    lax.fori_loop(0, nc, start_q, 0)
    lax.fori_loop(0, nc, start_kv, 0)

    barrier = pltpu.get_barrier_semaphore()
    peers = (partner, ypeer, z1, z2, z3)
    for dev in peers:
        pl.semaphore_signal(barrier, inc=1, device_id={"dup": dev}, device_id_type=MESH)

    rowid = lax.broadcasted_iota(jnp.int32, (rows, span), 0)
    lane = lax.broadcasted_iota(jnp.int32, (rows, span), 1)
    slot = (rowid * 171) >> 9
    item = rowid - 3 * slot
    rel = (slot & 3) * 4 + ((slot >> 2) & 1) * 2 + (slot >> 3)
    tok = (own * (rel ^ me) + item) & 3
    posm[...] = me * span + lane + 4 - tok
    ltmp[...] = jnp.zeros_like(ltmp)

    pltpu.make_async_copy(q_ref, q_ref, qsem).wait()
    pl.semaphore_wait(barrier, len(peers))

    def q_far(c, ny):
        y = upto(ny)
        send(qbuf.at[c, 0, y, 0], qbuf.at[c, 0, y, 2 + inner], ny + ny - 1, rq.at[1, c], far_inner)
        pl.when(inner == 0)(lambda: q_near(c, ny))

    def q_near(c, ny):
        y = upto(ny)
        send(qbuf.at[c, 0, y, 0], qbuf.at[c, 0, y, 1], ny + ny - 1, rq.at[0, c], z1)

    def q_relayed(c, ny):
        recv(qbuf.at[c, 0, upto(ny), pl.ds(2, 2)], rq.at[1, c])

    def q_relay(c, ny):
        @pl.when(inner == 1)
        def _():
            y = upto(ny)
            q_relayed(c, ny)
            send(qbuf.at[c, 0, y, 2], qbuf.at[c, 0, y, 3], 2 * ny, rq.at[1, c], z1)
            send(qbuf.at[c, 0, y, 3], qbuf.at[c, 0, y, 2], 2 * ny, rq.at[1, c], z1)
            q_near(c, ny)

    def q_end(c, ny):
        pl.when(inner == 0)(lambda: q_relayed(c, ny))
        recv(qbuf.at[c, 0, upto(ny), 1], rq.at[0, c])

    def q_y_own(c, si=5):
        send(qbuf.at[c, 0, 0, 0], qbuf.at[c, 0, 1, 0], si, rq.at[2, c], ypeer)

    def q_y_rest(c):
        z = pl.ds(1, 3)
        send(qbuf.at[c, 0, 0, z], qbuf.at[c, 0, 1, z], 5, rq.at[2, c], ypeer)

    def q_y_if(c, role):
        @pl.when(inner == role)
        def _():
            q_end(c, 1)
            q_y_rest(c)

    def q_partner(c):
        send(qbuf.at[c, 0], qbuf.at[c, 1], 7, rq.at[3, c], partner)

    def q_last(c):
        recv(qbuf.at[c, 0, 1], rq.at[2, c])
        q_partner(c)

    def both(*fns):
        def run(c):
            for fn in fns:
                fn(c)
        return run

    y_own = by_way(Q_WAY, {"A": q_y_own, "B": lambda c: q_y_own(c, 6)})
    q0 = by_way(Q_WAY, {"A": lambda c: q_far(c, 1)})
    q1 = by_way(Q_WAY, {
        "A": both(lambda c: q_relay(c, 1), lambda c: q_y_if(c, 1)),
        "B": both(lambda c: recv(qbuf.at[c, 0, 1, 0], rq.at[2, c]), lambda c: q_far(c, 2))})
    q2 = by_way(Q_WAY, {
        "A": lambda c: q_y_if(c, 0),
        "B": lambda c: q_relay(c, 2)})
    q3 = by_way(Q_WAY, {
        "A": q_last,
        "B": both(lambda c: q_end(c, 2), q_partner)})

    def compute(c):
        recv(qbuf.at[c, 1], rq.at[3, c])
        for s in range(16):
            for i in range(own):
                qf[pl.ds((s * own + i) * pitch, bc), :] = qbuf[c, s // 8, (s // 4) % 2, s % 4, i].astype(F32)
        pltpu.make_async_copy(k_ref.at[pl.ds(0, 2 * bc)], kbuf.at[pl.ds(0, 2 * bc)], kvsem.at[c]).wait()
        base = (c % 2) * (rows * pitch)
        macc[...] = jnp.zeros_like(macc)
        dacc[...] = jnp.zeros_like(dacc)
        place = lax.broadcasted_iota(jnp.int32, (rows, 128), 1)
        rid = lax.broadcasted_iota(jnp.int32, (rows, 128), 0)
        place = place - bc * (rid - 3 * ((rid * 171) >> 9))

        def scores(j):
            qb = qf[pl.ds(j, rows, stride=pitch), :].astype(BF16)
            sbuf[j] = lax.dot_general(qb, kbuf[c * bc + j], (((1,), (1,)), ((), ())), preferred_element_type=F32)

        def soften(j, mv, dv):
            s = jnp.where(posm[...] <= len_ref[c * bc + j], sbuf[j], NEG)
            mx = jnp.maximum(jnp.max(s, axis=1, keepdims=True), FLOOR)
            p = jnp.exp2((s - mx) * (scale * math.log2(math.e)))
            pbuf[j] = p.astype(BF16)
            hit = place == j
            return jnp.where(hit, mx, mv), jnp.where(hit, jnp.sum(p, axis=1, keepdims=True), dv)

        def soften_group(g, carry):
            mv, dv = macc[...], dacc[...]
            for u in range(UNROLL):
                mv, dv = soften(g * UNROLL + u, mv, dv)
            macc[...] = mv
            dacc[...] = dv
            return carry

        for j in range(bc):
            scores(j)
        lax.fori_loop(0, bc // UNROLL, soften_group, 0)
        for j in range(bc):
            of[pl.ds(base + j, rows, stride=pitch), :] = jnp.dot(pbuf[j], vbuf[c * bc + j], preferred_element_type=F32)
        for t, acc in ((0, macc), (1, dacc)):
            line = acc[pl.ds(0, 16, stride=3), :] + acc[pl.ds(1, 16, stride=3), :] + acc[pl.ds(2, 16, stride=3), :]
            if t == 0:
                line = line * scale
            e1k[c, t] = line[:8]
            e1s[c, t] = line[8:]
        for r in range(half):
            p1s[c, r] = of[pl.ds(base + (half + r) * pitch, bc), :].astype(BF16)
        send(e1s.at[c], e1r.at[c], 9, rr.at[1, c], partner)
        send(p1s.at[c], p1r.at[c], 8, rr.at[0, c], partner)

    def finish(c, i, o):
        obuf[c, i] = o.astype(BF16)

    def ship(c):
        pltpu.make_async_copy(obuf.at[c], out_ref.at[:, pl.ds(c * bc, bc)], osem).start()

    def cut(w, line, i):
        return w[i * bc:(i + 1) * bc, line:line + 1]

    def lines(refs):
        for n, ref in refs:
            ltmp[n:n + 1] = ref
        return ltmp[...]

    def weights(*ls):
        top = functools.reduce(jnp.maximum, ls)
        es = [jnp.exp(x - top) for x in ls]
        tot = functools.reduce(lambda a, b: a + b, es)
        inv = 1.0 / tot
        return [(e * inv).T for e in es], top + jnp.log(tot)

    def merge_partner(c):
        recv(e1r.at[c], rr.at[1, c])
        ma, mb = e1k[c, 0], e1r[c, 0]
        top = jnp.maximum(ma, mb)
        ea, eb = jnp.exp(ma - top), jnp.exp(mb - top)
        tot = jnp.maximum(ea * e1k[c, 1] + eb * e1r[c, 1], 1.0)
        inv = 1.0 / tot
        lse[c] = top + jnp.log(tot)
        wa, wb = (ea * inv).T, (eb * inv).T
        recv(p1r.at[c], rr.at[0, c])
        base = (c % 2) * (rows * pitch)
        for n in range(8):
            for i in range(own):
                r = n * own + i
                part[c, n, i] = (cut(wa, n, i) * of[pl.ds(base + r * pitch, bc), :]
                                 + cut(wb, n, i) * p1r[c, r].astype(F32))

    def y_send(c, ny):
        for z in range(4 if ny == 1 else 1):
            eys[c, z] = lse[c, 4 + z:5 + z]
            for i in range(own):
                ys[c, z, i] = part[c, 4 + z, i].astype(BF16)
        if ny == 1:
            send(eys.at[c], eyr.at[c], 11, rr.at[3, c], ypeer)
            send(ys.at[c], yr.at[c], 10, rr.at[2, c], ypeer)
        else:
            send(eys.at[c, 0], eyr.at[c, 0], 13, rr.at[3, c], ypeer)
            send(ys.at[c, 0], yr.at[c, 0], 12, rr.at[2, c], ypeer)

    def y_merge(c, ny):
        if ny == 1:
            recv(eyr.at[c], rr.at[3, c])
            (wa, wb), new = weights(lse[c], lines([(z, eyr[c, z]) for z in range(4)]))
            lse[c] = new
            recv(yr.at[c], rr.at[2, c])
            for z in range(4):
                for i in range(own):
                    part[c, z, i] = cut(wa, z, i) * part[c, z, i] + cut(wb, z, i) * yr[c, z, i].astype(F32)
        else:
            recv(eyr.at[c, 0], rr.at[3, c])
            (wa, wb), _ = weights(lse[c], lines([(0, eyr[c, 0])]))
            recv(yr.at[c, 0], rr.at[2, c])
            for i in range(own):
                finish(c, i, cut(wa, 0, i) * part[c, 0, i] + cut(wb, 0, i) * yr[c, 0, i].astype(F32))
            ship(c)

    def z_send(c, ny):
        y = upto(ny)
        for k, dat, lin in ((3, zos.at[c, 1], eos.at[c, 1]), (2, zos.at[c, 0], eos.at[c, 0]), (1, zns.at[c], ens.at[c])):
            for h in range(ny):
                lin[h] = lse[c, 4 * h + k:4 * h + k + 1]
                for i in range(own):
                    dat[h, i] = part[c, 4 * h + k, i].astype(BF16)
        for m, dev in ((1, z3), (0, z2)):
            send(eos.at[c, m, y], eor.at[c, m, y], 17 + ny + ny, rr.at[7, c], dev)
            send(zos.at[c, m, y], zor.at[c, m, y], 16 + ny + ny, rr.at[6, c], dev)
        send(ens.at[c, y], enr.at[c, y], 13 + ny + ny, rr.at[5, c], z1)
        send(zns.at[c, y], znr.at[c, y], 12 + ny + ny, rr.at[4, c], z1)

    def z_merge(c, ny):
        y = upto(ny)
        recv(enr.at[c, y], rr.at[5, c])
        recv(eor.at[c, :, y], rr.at[7, c])
        came = ((znr.at[c], enr.at[c]), (zor.at[c, 0], eor.at[c, 0]), (zor.at[c, 1], eor.at[c, 1]))
        ws, new = weights(lse[c], *[lines([(4 * h, lin[h]) for h in range(ny)]) for _, lin in came])
        recv(znr.at[c, y], rr.at[4, c])
        recv(zor.at[c, :, y], rr.at[6, c])
        for h in range(ny):
            for i in range(own):
                o = cut(ws[0], 4 * h, i) * part[c, 4 * h, i]
                for w, (dat, _) in zip(ws[1:], came):
                    o = o + cut(w, 4 * h, i) * dat[h, i].astype(F32)
                if ny == 1:
                    finish(c, i, o)
                else:
                    part[c, 4 * h, i] = o
        if ny == 1:
            ship(c)
        else:
            lse[c] = new

    r0_send = by_way(O_WAY, {"D": lambda c: y_send(c, 1), "E": lambda c: z_send(c, 2)})

    def r0(c):
        merge_partner(c)
        r0_send(c)

    r1 = by_way(O_WAY, {
        "D": both(lambda c: y_merge(c, 1), lambda c: z_send(c, 1)),
        "E": both(lambda c: z_merge(c, 2), lambda c: y_send(c, 2))})
    r2 = by_way(O_WAY, {"D": lambda c: z_merge(c, 1), "E": lambda c: y_merge(c, 2)})

    def at(c, fn):
        pl.when((c >= 0) & (c < nc))(lambda: fn(c))

    def first(c, carry):
        pl.when(c < AHEAD)(lambda: q0(c))
        y_own(c)
        return carry

    lax.fori_loop(0, Y_AHEAD, first, 0)

    def step(st, carry):
        at(st + AHEAD, q0)
        at(st + Y_AHEAD, y_own)
        at(st - LAG[0], q1)
        at(st - LAG[1], q2)
        at(st - LAG[2], q3)
        at(st - LAG[3], compute)
        at(st - LAG[4], r0)
        at(st - LAG[5], r1)
        at(st - LAG[6], r2)
        return carry

    lax.fori_loop(0, nc + LAG[6], step, 0)

    def sent(ref, si):
        remote(ref, ref, ss.at[si], rq.at[0, 0], partner).wait_send()

    def sent_of(n, *pairs):
        if n:
            for fn, si in pairs:
                sent(fn(upto(n)), si)

    na, nbb = (Q_WAY.count(w) for w in "AB")
    sent_of(na, (lambda c: qbuf.at[c, 0, 0, upto(2)], 1))
    sent_of(nbb, (lambda c: qbuf.at[c, 0, :, upto(2)], 3), (lambda c: qbuf.at[c, 0, 0, 0], 6))
    sent_of(na, (lambda c: qbuf.at[c, 0, 0], 5))

    @pl.when(inner == 1)
    def _():
        sent_of(na, (lambda c: qbuf.at[c, 0, 0, upto(2)], 2))
        sent_of(nbb, (lambda c: qbuf.at[c, 0, :, upto(2)], 4))

    sent(qbuf.at[:, 0], 7)
    od, oe = (O_WAY.count(w) for w in "DE")
    sent_of(od, (lambda c: ys.at[c], 10), (lambda c: eys.at[c], 11),
            (lambda c: zns.at[c, 0], 14), (lambda c: ens.at[c, 0], 15),
            (lambda c: zos.at[c, :, 0], 18), (lambda c: eos.at[c, :, 0], 19))
    sent_of(oe, (lambda c: ys.at[c, 0], 12), (lambda c: eys.at[c, 0], 13),
            (lambda c: zns.at[c], 16), (lambda c: ens.at[c], 17),
            (lambda c: zos.at[c], 20), (lambda c: eos.at[c], 21))

    sent(p1s, 8)
    sent(e1s, 9)
    pltpu.make_async_copy(out_ref, out_ref, osem).wait()


def solution(mesh):
    def group_step(q_local, k_span, v_span, len_local):
        nb, own, dim = q_local.shape
        span = k_span.shape[1]
        rows = 16 * own
        half = rows // 2
        nc = CHUNKS
        bc = nb // nc
        pitch = bc + 8
        q_planes = jnp.transpose(q_local, (1, 0, 2))
        vm = pltpu.VMEM
        dma = pltpu.SemaphoreType.DMA
        any_spec = pl.BlockSpec(memory_space=pl.ANY)

        def blocks(*lead):
            return vm((nc, *lead, own, bc, dim), BF16)

        def line(*lead):
            return vm((nc, *lead, 1, 128), F32)

        out = pl.pallas_call(
            functools.partial(fused, nb, own, span, dim),
            out_shape=jax.ShapeDtypeStruct((own, nb, dim), BF16),
            in_specs=[pl.BlockSpec(memory_space=pltpu.SMEM), any_spec, any_spec, any_spec],
            out_specs=any_spec,
            scratch_shapes=[
                vm((nb, span, dim), BF16), vm((nb, span, dim), BF16),
                blocks(2, 2, 4),
                vm((rows * pitch, dim), F32), vm((2 * rows * pitch, dim), F32),
                vm((rows, span), jnp.int32), vm((rows, 128), F32), vm((rows, 128), F32),
                vm((bc, rows, span), F32), vm((bc, rows, span), BF16),
                vm((nc, half, bc, dim), BF16), vm((nc, half, bc, dim), BF16),
                vm((nc, 2, 8, 128), F32), vm((nc, 2, 8, 128), F32), vm((nc, 2, 8, 128), F32),
                vm((nc, 8, own, bc, dim), F32), vm((nc, 8, 128), F32), vm((8, 128), F32),
                blocks(4), blocks(4), blocks(2), blocks(2),
                blocks(2, 2), blocks(2, 2),
                line(4), line(4), line(2), line(2), line(2, 2), line(2, 2),
                blocks(), dma((nc,)), dma, dma, dma((22,)), dma((4, nc)), dma((8, nc)),
            ],
            compiler_params=pltpu.CompilerParams(
                collective_id=0, has_side_effects=True, vmem_limit_bytes=67043328),
            name="attend",
        )(len_local, q_planes, k_span, v_span)
        return jnp.transpose(out, (1, 0, 2))

    return jax.shard_map(group_step, mesh=mesh, in_specs=(P("kv", "dup", None), P("kv", "dup", None), P("kv", "dup", None), P("kv")), out_specs=P("kv", "dup", None), check_vma=False)
```
